32 devices in a mesh: lon: 16 (over z, y, x), lev: 2 (over core).
Axes of the slice: x: 2, y: 2, z: 4, core: 2. Of those that a mesh axis runs over, the one named last changes fastest.
Arguments:
- ensemble: float32 [80, 16, 16384], P(None, 'lev', 'lon'), may hold values from -6 to 6
- obs_cell: int32 [12, 128], P(None, 'lon'), may hold values from 0 to 16383, as said below
- obs_value: float32 [12, 128], P(None, 'lon'), may hold values from -5 to 5
- obs_noise: float32 [12, 128], P(None, 'lon'), may hold values from 0.2 to 2
- obs_weight: float32 [12, 16, 128], P(None, 'lev'), may hold values from 0.05 to 0.5
- tile_lists: int32 [12, 384], P(None, 'lon'), may hold values from 0 to 128, as said below
- batch_order: int32 [12], replicated, may hold values from 0 to 11, each once
Outputs:
- analysis: float32 [80, 16, 16384], P(None, 'lev', 'lon')
The draws below stay inside these ranges and needn't reach their ends.
Inputs may be any that keep to these rules, and one draw needn't show every extreme that they name: `obs_cell`: each tile holds at most 8 observations of one block, and some tile exactly 8. `tile_lists`: for block b and tile t the tile's 24 slots hold first, ascending and once each, the observations of block b whose tile is t or a neighbour of t around the globe, then the value 128 in every remaining slot; in every block some tile has all 24 slots used. `batch_order`: each block once.
All inputs are finite; a program needn't handle non-finite values.
Results may differ from the reference program's by a relative error of at most 0.0003.
Values sent between devices are 32-bit elements; how exact they have to be, the bound alone decides.
A program may use at most 128 MiB of HBM per device.

```python
import math
import jax
import jax.numpy as jnp
from jax import lax

MEM = 80
OBS = 128
OWN_MAX = 8
ROUTE_CAP = 24
LON_DEV = 16
CELL_DEV = 1024
BATCHES = 12
LEVELS = 16
CELLS = 16384
N_LON = 16


def block_layout(key):
    subkeys = jax.random.split(jax.random.fold_in(key, 7351), BATCHES)

    def single(subkey):
        pick_key = jax.random.fold_in(subkey, 0)
        order_key = jax.random.fold_in(subkey, 1)
        cell_key = jax.random.fold_in(subkey, 2)
        shuffle_key = jax.random.fold_in(subkey, 4)
        slot_count = N_LON * OWN_MAX
        slot_tile = jnp.arange(slot_count, dtype=jnp.int32) // OWN_MAX
        centre = jax.random.randint(pick_key, (), 0, N_LON)
        forward = (slot_tile - centre) % N_LON
        backward = (centre - slot_tile) % N_LON
        nearby = (jnp.minimum(forward, backward) <= 1).astype(jnp.int32)
        score = jax.random.permutation(order_key, slot_count).astype(jnp.int32) + nearby * slot_count
        chosen = lax.top_k(score, OBS)[1].astype(jnp.int32)
        chosen = jax.random.permutation(shuffle_key, chosen)
        tiles = slot_tile[chosen]
        cell_ids = tiles * CELL_DEV + jax.random.randint(cell_key, (OBS,), 0, CELL_DEV)
        tile_ids = jnp.arange(N_LON, dtype=jnp.int32)
        distance_tiles = (tiles[None, :] - tile_ids[:, None]) % N_LON
        reached = (distance_tiles <= 1) | (distance_tiles == N_LON - 1)
        total = jnp.sum(reached.astype(jnp.int32), axis=1)
        numbers = jnp.arange(OBS, dtype=jnp.int32)
        ordering = jnp.where(reached, numbers[None, :], numbers[None, :] + OBS)
        ordered = jnp.argsort(ordering, axis=1, stable=True)[:, :ROUTE_CAP].astype(jnp.int32)
        slot_ids = jnp.arange(ROUTE_CAP, dtype=jnp.int32)
        lists = jnp.where(slot_ids[None, :] < total[:, None], ordered, OBS)
        return (cell_ids, lists.reshape(-1).astype(jnp.int32))
    return jax.vmap(single)(subkeys)


def draw_obs_cell(key, part):
    return block_layout(key)[0]


def draw_tile_lists(key, part):
    return block_layout(key)[1]


def shard_levels(stream_key, shape, cuts, least, top_value):
    gain, own = 1.0, jax.random.fold_in(stream_key, 6)
    for axis_at, parts in cuts:
        draws = jnp.exp(jax.random.uniform(jax.random.fold_in(own, axis_at), (parts,), jnp.float32, least / len(cuts), top_value / len(cuts)))
        gain = gain * jnp.repeat(draws, shape[axis_at] // parts).reshape([-1 if axis == axis_at else 1 for axis in range(len(shape))])
    return gain


def normal_values(key, extent, scale, limit, shards=(), held_as=jnp.bfloat16):
    entries = jax.random.normal(key, extent, jnp.float32) * scale
    if len(shards) > 0:
        entries = shard_levels(key, extent, shards, -0.22, 0.18) * entries
    return jnp.clip(entries, min=-limit, max=limit).astype(held_as)


def setup_inputs(seed: int = 0) -> dict:
    streams_of = jax.random.split(jax.random.key(seed), 8)
    return {
        "ensemble": normal_values(streams_of[0], (MEM, LEVELS, CELLS), 1.0, 6.0, ((1, 2), (2, 16)), jnp.float32),
        "obs_cell": draw_obs_cell(jax.random.fold_in(streams_of[7], 71), 0),
        "obs_value": normal_values(streams_of[2], (BATCHES, OBS), 1.0, 5.0, ((1, 16),), jnp.float32),
        "obs_noise": jnp.clip(jnp.exp(math.log(2.0) - 2.3025851 * jax.random.uniform(streams_of[3], (BATCHES, OBS), jnp.float32) ** shard_levels(streams_of[3], (BATCHES, OBS), ((1, 16),), -0.2, 0.2)), 0.2, 2.0),
        "obs_weight": jnp.clip(jnp.exp(math.log(0.5) - 2.3025851 * jax.random.uniform(streams_of[4], (BATCHES, LEVELS, OBS), jnp.float32) ** shard_levels(streams_of[4], (BATCHES, LEVELS, OBS), ((1, 2),), -0.2, 0.2)), 0.05, 0.5),
        "tile_lists": draw_tile_lists(jax.random.fold_in(streams_of[7], 71), 0),
        "batch_order": jax.random.permutation(streams_of[6], BATCHES).astype(jnp.int32),
    }


highest = lax.Precision.HIGHEST

def locate(cell_ids):
    within = cell_ids % CELL_DEV
    return (within // LON_DEV, cell_ids // CELL_DEV * LON_DEV + within % LON_DEV)

def taper_weight(source_ids, target_ids, circle):
    source_row, source_col = locate(source_ids)
    target_row, target_col = locate(target_ids)
    apart_cols = jnp.abs(source_col[:, None] - target_col[None, :])
    apart_cols = jnp.minimum(apart_cols, circle - apart_cols)
    apart_rows = source_row[:, None] - target_row[None, :]
    square = (apart_cols * apart_cols + apart_rows * apart_rows).astype(jnp.float32)
    return jnp.exp(square * (-2.0 / (LON_DEV * LON_DEV)))

def gain_parts(sample_now, observed, noise):
    centre = lax.optimization_barrier(jnp.mean(sample_now, axis=0))
    spread = sample_now - centre
    covariance = jnp.dot(spread.T, spread, precision=highest) / (MEM - 1) + jnp.diag(noise)
    factor = jnp.linalg.cholesky(covariance)
    innovation = (observed - centre)[:, None]
    halfway = lax.linalg.triangular_solve(factor, innovation, left_side=True, lower=True)
    kalman_gain = lax.linalg.triangular_solve(factor, halfway, left_side=True, lower=True, transpose_a=True)[:, 0]
    rooted = factor + jnp.diag(jnp.sqrt(noise))
    identity = jnp.eye(OBS, dtype=noise.dtype)
    within = lax.linalg.triangular_solve(rooted, identity, left_side=True, lower=True)
    reduced = lax.linalg.triangular_solve(factor, within, left_side=True, lower=True, transpose_a=True)
    return (spread, kalman_gain, reduced)

def update_block(block, spread, kalman_gain, reduced, chosen, usable, obs_ids, local_ids, circle):
    levels = block.shape[1]
    rows_used = chosen.shape[0]
    weight = taper_weight(obs_ids[chosen], local_ids, circle) * usable[:, None]
    centre = lax.optimization_barrier(jnp.mean(block, axis=0))
    flattened = (block - centre).reshape(MEM, -1)
    crossed = jnp.dot(spread[:, chosen].T, flattened, precision=highest) / (MEM - 1)
    tapered = (crossed.reshape(rows_used, levels, -1) * weight[:, None, :]).reshape(rows_used, -1)
    shifted = jnp.dot(kalman_gain[chosen], tapered, precision=highest)
    mixing = jnp.dot(spread, reduced[chosen].T, precision=highest)
    flattened = flattened - jnp.dot(mixing, tapered, precision=highest)
    return ((centre.reshape(-1) + shifted)[None, :] + flattened).reshape(block.shape)

def reference(ensemble, obs_cell, obs_value, obs_noise, obs_weight, tile_lists, batch_order):
    circle = LON_DEV * N_LON
    tiles = ensemble.reshape(MEM, LEVELS, N_LON, CELL_DEV).transpose(2, 0, 1, 3)
    tile_ids = jnp.arange(N_LON, dtype=jnp.int32)

    def serial(tiles, position):
        current = batch_order[position]
        cell_ids = obs_cell[current]
        owners = cell_ids // CELL_DEV
        within = cell_ids % CELL_DEV
        picked = tiles[owners, :, :, within]
        probe = lax.optimization_barrier(jnp.sum(picked * obs_weight[current].T[:, None, :], axis=2)).T
        spread, kalman_gain, reduced = gain_parts(probe, obs_value[current], obs_noise[current])
        lists = tile_lists[current].reshape(N_LON, ROUTE_CAP)
        filled = (lists < OBS).astype(jnp.float32)
        safe = jnp.minimum(lists, OBS - 1).astype(jnp.int32)

        def single(items):
            block, chosen, usable, tile_index = items
            local_ids = tile_index * CELL_DEV + jnp.arange(CELL_DEV, dtype=jnp.int32)
            return update_block(block, spread, kalman_gain, reduced, chosen, usable, cell_ids, local_ids, circle)
        tiles = lax.map(single, (tiles, safe, filled, tile_ids))
        return (tiles, None)
    tiles, unused = lax.scan(serial, tiles, jnp.arange(BATCHES, dtype=jnp.int32))
    return tiles.transpose(1, 2, 0, 3).reshape(MEM, LEVELS, CELLS)
```

```python
import functools

import jax
import jax.numpy as jnp
from jax import lax
from jax.experimental import pallas as pl
from jax.experimental.pallas import tpu as pltpu
from jax.sharding import PartitionSpec as P

LON_DEV = 16
CELL_DEV = 1024
PANEL = 16

highest = lax.Precision.HIGHEST
f32 = jnp.float32
bf16 = jnp.bfloat16


def split(x):
    high = x.astype(bf16)
    low = (x - high.astype(f32)).astype(bf16)
    return high, low


def dot(a, b):
    return jnp.dot(a, b, preferred_element_type=f32)


def tapered_weight(row_a, col_a, row_c, col_c, circle):
    e = jnp.abs(col_a - col_c)
    e = jnp.minimum(e, circle - e)
    d = row_a - row_c
    return jnp.exp((e * e + d * d) * (-2.0 / (LON_DEV * LON_DEV)))


def eliminate(a_ref, b_ref, noise_root, mem, obs, width, beside):
    lane = lax.broadcasted_iota(jnp.int32, (1, obs), 1)
    sample = lax.broadcasted_iota(jnp.int32, (1, width), 1) < mem
    for start in range(0, obs, PANEL):
        spot = [[None] * PANEL for _ in range(PANEL)]
        for i in range(PANEL):
            for s in range(i + 1):
                spot[i][s] = jnp.broadcast_to(
                    a_ref[start + i : start + i + 1, start + s : start + s + 1], (1, obs)
                )
        in_panel = (lane >= start) & (lane < start + PANEL)
        rows = []
        sides = []
        for i in range(PANEL):
            row = a_ref[start + i : start + i + 1, :]
            rows.append(jnp.where(in_panel, jnp.where(lane == start + i, 1.0, 0.0), row))
            sides.append(b_ref[start + i : start + i + 1, :])
        scaled_rows = []
        scaled_sides = []
        for r in range(PANEL):
            pivot = spot[r][r]
            inverse_root = lax.rsqrt(pivot)
            inverse = inverse_root * inverse_root
            root = pivot * inverse_root
            added = jnp.where(sample, noise_root[start + r], 0.0)
            factor = 1.0 / (root + added)
            below = [spot[i][r] * inverse for i in range(r + 1, PANEL)]
            for n, i in enumerate(range(r + 1, PANEL)):
                for s in range(r + 1, i + 1):
                    spot[i][s] = spot[i][s] - below[n] * spot[s][r]
            solved = sides[r] * factor
            passing = solved * root
            for n, i in enumerate(range(r + 1, PANEL)):
                rows[i] = rows[i] - below[n] * rows[r]
                sides[i] = sides[i] - below[n] * passing
            scaled_rows.append(rows[r] * inverse)
            scaled_sides.append(solved * inverse_root)
            a_ref[start + r : start + r + 1, :] = jnp.where(
                lane < start + PANEL, rows[r] * inverse_root, 0.0
            )
            b_ref[start + r : start + r + 1, :] = solved
        beside(start // PANEL, obs // PANEL)
        after = start + PANEL
        if after < obs:
            u_high, u_low = split(jnp.concatenate(rows, axis=0))
            high, low = split(jnp.concatenate(
                [jnp.concatenate(scaled_rows, axis=0), jnp.concatenate(scaled_sides, axis=0)], axis=1
            ))
            upper = jnp.concatenate([u_high.astype(f32), u_high.astype(f32), u_low.astype(f32)], axis=0)
            left = upper.T.astype(bf16)[after:, :]
            change = dot(left, jnp.concatenate([high, low, high], axis=0))
            a_ref[after:, :] = jnp.where(in_panel, 0.0, a_ref[after:, :]) - change[:, :obs]
            b_ref[after:, :] = b_ref[after:, :] - change[:, obs:]


def kernel_body(
    x_ref, probe_ref, value_ref, noise_ref, noise_col_ref, cell_row_ref, cell_col_ref, list_ref,
    out_ref, probes, a_ref, b_ref, weight_ref, left_ref, gains_ref, *, batches, levels, mem, obs, cells, slots, axis_size,
):
    tile = lax.axis_index("lon")
    circle = float(LON_DEV * axis_size)
    scale = 1.0 / (mem - 1)
    probes[...] = probe_ref[...]
    cell = lax.broadcasted_iota(jnp.int32, (1, cells), 1)
    here_row = (cell // LON_DEV).astype(f32)
    here_col = (tile * LON_DEV + cell % LON_DEV).astype(f32)
    target = cell_row_ref[...]
    target_tile = target // CELL_DEV
    target_within = target - target_tile * CELL_DEV
    target_row_int = target_within // LON_DEV
    target_col = (target_tile * LON_DEV + target_within - target_row_int * LON_DEV).astype(f32)
    target_row = target_row_int.astype(f32)
    target_tile = target_tile.astype(f32)
    lanes = lax.broadcasted_iota(jnp.int32, (obs, obs), 1)
    subs = lax.broadcasted_iota(jnp.int32, (obs, obs), 0)

    def spread_piece(level, start, width):
        piece = pl.ds(start, width)
        block = out_ref[level, :, piece]
        high, low = split(block)
        crossed = dot(left_ref[...], jnp.concatenate([high, low, high], axis=0))
        high, low = split(crossed * weight_ref[:, piece])
        out_ref[level, :, piece] = block + dot(gains_ref[...], jnp.concatenate([high, low, high], axis=0))

    def beside(step, steps):
        halves = 2 * levels
        for piece in range(step * halves // steps, (step + 1) * halves // steps):
            spread_piece(piece // 2, piece % 2 * (cells // 2), cells // 2)

    def turn(k, carry):
        now = probes[k]
        centre = jnp.mean(now, axis=0, keepdims=True)
        spread = now - centre
        innovation = value_ref[k] - centre
        padded = jnp.concatenate(
            [spread, innovation, jnp.zeros((obs - mem - 1, obs), f32)], axis=0
        )
        sides = padded.T
        noise_row = noise_ref[k]
        covariance = jnp.dot(sides[:, :mem], spread, precision=highest, preferred_element_type=f32) * scale
        a_ref[...] = covariance + jnp.where(lanes == subs, noise_row, 0.0)
        b_ref[...] = sides
        root_col = jnp.sqrt(noise_col_ref[k])
        roots = [root_col[j : j + 1, :] for j in range(obs)]
        eliminate(a_ref, b_ref, roots, mem, obs, obs, beside)
        joined = lax.dot_general(
            a_ref[...], b_ref[...], (((0,), (0,)), ((), ())), precision=highest, preferred_element_type=f32
        )
        gain_t = joined[:, mem : mem + 1] - joined
        gain = gain_t.T[:mem, :]

        s_high, s_low = split(spread)
        stacked = jnp.concatenate([s_high.astype(f32), s_high.astype(f32), s_low.astype(f32)], axis=0)
        left = stacked.T.astype(bf16)
        g_high, g_low = split(gain)
        gains = jnp.concatenate([g_high, g_high, g_low], axis=1)

        cell_col = cell_col_ref[k]
        from_tile = cell_col // CELL_DEV
        from_within = cell_col - from_tile * CELL_DEV
        from_row = from_within // LON_DEV
        from_col = (from_tile * LON_DEV + from_within - from_row * LON_DEV).astype(f32)
        from_row = from_row.astype(f32)
        from_tile = from_tile.astype(f32)

        def renew(b, carry):
            @pl.when(2 * b + 1 > k)
            def _():
                upcoming = jnp.concatenate([probes[2 * b], probes[2 * b + 1]], axis=1)
                high, low = split(upcoming)
                crossed = dot(left, jnp.concatenate([high, low, high], axis=0))
                weights = []
                for u in range(2):
                    weight = tapered_weight(
                        from_row, from_col, target_row_ref_get(b, u), target_col_ref_get(b, u), circle
                    )
                    apart = jnp.abs(from_tile - target_tile_ref_get(b, u))
                    near = (apart < 1.5) | (apart > axis_size - 1.5)
                    weights.append(jnp.where(near, weight * scale, 0.0))
                tapered = crossed * jnp.concatenate(weights, axis=1)
                high, low = split(tapered)
                upcoming = upcoming + dot(gains, jnp.concatenate([high, low, high], axis=0))
                probes[2 * b] = upcoming[:, :obs]
                probes[2 * b + 1] = upcoming[:, obs:]

            return carry

        def target_row_ref_get(b, u):
            return target_row[2 * b + u]

        def target_col_ref_get(b, u):
            return target_col[2 * b + u]

        def target_tile_ref_get(b, u):
            return target_tile[2 * b + u]

        for b in range(batches // 2):
            renew(b, 0)

        listed = list_ref[k]
        chosen = lanes[:slots] == listed
        select = chosen.astype(bf16)
        pick_row = cell_row_ref[k]
        pick_tile = pick_row // CELL_DEV
        pick_within = pick_row - pick_tile * CELL_DEV
        pick_r = pick_within // LON_DEV
        pick_c = (pick_tile * LON_DEV + pick_within - pick_r * LON_DEV).astype(f32)
        list_row = jnp.sum(jnp.where(chosen, pick_r.astype(f32), 0.0), axis=1, keepdims=True)
        list_col = jnp.sum(jnp.where(chosen, pick_c, 0.0), axis=1, keepdims=True)
        usable = jnp.where(listed < obs, scale, 0.0)
        weight = tapered_weight(list_row, list_col, here_row, here_col, circle) * usable
        left_listed = dot(select, left).astype(bf16)
        gt_high, gt_low = split(gain_t)
        gt_high = dot(select, gt_high)
        gt_low = dot(select, gt_low)
        gains_listed = jnp.concatenate([gt_high, gt_high, gt_low, jnp.zeros((obs - 3 * slots, obs), f32)], axis=0)
        gains_listed = gains_listed.T[:mem, : 3 * slots].astype(bf16)

        weight_ref[...] = weight
        left_ref[...] = left_listed
        gains_ref[...] = gains_listed
        return carry

    out_ref[...] = x_ref[...]
    weight_ref[...] = jnp.zeros(weight_ref.shape, f32)
    left_ref[...] = jnp.zeros(left_ref.shape, bf16)
    gains_ref[...] = jnp.zeros(gains_ref.shape, bf16)
    lax.fori_loop(0, batches, turn, 0)

    def last(level, carry):
        spread_piece(level, 0, cells)
        return carry

    lax.fori_loop(0, levels, last, 0)


def peer_of(d, ranks, both):
    lon, lev = lax.axis_index("lon"), lax.axis_index("lev")
    if not both:
        return lax.rem(lon + d, ranks), lev
    cores = lax.axis_size("lev")
    number = lax.rem(lon * cores + lev + d, ranks)
    return lax.div(number, cores), lax.rem(number, cores)


def meet(ranks, both):
    barrier = pltpu.get_barrier_semaphore()

    def announce(d, carry):
        pl.semaphore_signal(
            barrier, inc=1, device_id=peer_of(d, ranks, both), device_id_type=pl.DeviceIdType.MESH
        )
        return carry

    lax.fori_loop(1, ranks, announce, 0)
    pl.semaphore_wait(barrier, ranks - 1)


def each_peer(ranks, copy_to):
    def start(d, carry):
        copy_to(d).start()
        return carry

    def finish(d, carry):
        copy_to(d).wait()
        return carry

    return (
        lambda: lax.fori_loop(1, ranks, start, 0),
        lambda: lax.fori_loop(1, ranks, finish, 0),
    )


def table_kernel(mine_ref, out_ref, landed, send_sem, recv_sem, *, ranks):
    meet(ranks, False)

    def copy_to(d):
        return pltpu.make_async_remote_copy(
            src_ref=mine_ref,
            dst_ref=landed.at[d],
            send_sem=send_sem.at[d],
            recv_sem=recv_sem.at[d],
            device_id=peer_of(d, ranks, False),
            device_id_type=pl.DeviceIdType.MESH,
        )

    start, finish = each_peer(ranks, copy_to)
    start()
    landed[0] = mine_ref[...]
    finish()
    out_ref[...] = jnp.sum(landed[...], axis=0)


def sum_kernel(mine_ref, out_ref, landed, total, send_sem, recv_sem, send_again, recv_again, *, ranks, rows):
    meet(ranks, True)
    me = lax.axis_index("lon") * lax.axis_size("lev") + lax.axis_index("lev")
    own = pl.ds(pl.multiple_of(me * rows, rows), rows)

    def scatter_to(d):
        other = lax.rem(me + d, ranks)
        return pltpu.make_async_remote_copy(
            src_ref=mine_ref.at[pl.ds(pl.multiple_of(other * rows, rows), rows)],
            dst_ref=landed.at[d],
            send_sem=send_sem.at[d],
            recv_sem=recv_sem.at[d],
            device_id=peer_of(d, ranks, True),
            device_id_type=pl.DeviceIdType.MESH,
        )

    def gather_to(d):
        return pltpu.make_async_remote_copy(
            src_ref=total,
            dst_ref=out_ref.at[own],
            send_sem=send_again.at[d],
            recv_sem=recv_again.at[d],
            device_id=peer_of(d, ranks, True),
            device_id_type=pl.DeviceIdType.MESH,
        )

    start, finish = each_peer(ranks, scatter_to)
    start()
    landed[0] = mine_ref[own]
    finish()
    total[...] = jnp.sum(landed[...], axis=0)
    start, finish = each_peer(ranks, gather_to)
    start()
    out_ref[own] = total[...]
    finish()


def gathered_table(parts, axis_size):
    rows, own = parts.shape
    padded = -(-rows // 8) * 8
    width = own * axis_size
    lane = jnp.arange(width, dtype=jnp.int32)[None, :]
    placed = jnp.where(lane // own == lax.axis_index("lon"), jnp.tile(parts, (1, axis_size)), 0.0)
    placed = jnp.pad(placed, ((0, padded - rows), (0, 0)))
    return pl.pallas_call(
        functools.partial(table_kernel, ranks=axis_size),
        out_shape=jax.ShapeDtypeStruct((padded, width), f32),
        in_specs=[pl.BlockSpec(memory_space=pltpu.VMEM)],
        out_specs=pl.BlockSpec(memory_space=pltpu.VMEM),
        scratch_shapes=[
            pltpu.VMEM((axis_size, padded, width), f32),
            pltpu.SemaphoreType.DMA((axis_size,)),
            pltpu.SemaphoreType.DMA((axis_size,)),
        ],
        compiler_params=pltpu.CompilerParams(collective_id=0, has_side_effects=True),
        name="table",
    )(placed)[:rows]


def summed(portions, ranks):
    count, width = portions.shape
    rows = -(-count // (8 * ranks)) * 8
    padded = jnp.pad(portions, ((0, rows * ranks - count), (0, 0)))
    return pl.pallas_call(
        functools.partial(sum_kernel, ranks=ranks, rows=rows),
        out_shape=jax.ShapeDtypeStruct(padded.shape, f32),
        in_specs=[pl.BlockSpec(memory_space=pltpu.VMEM)],
        out_specs=pl.BlockSpec(memory_space=pltpu.VMEM),
        scratch_shapes=[
            pltpu.VMEM((ranks, rows, width), f32),
            pltpu.VMEM((rows, width), f32),
            pltpu.SemaphoreType.DMA((ranks,)),
            pltpu.SemaphoreType.DMA((ranks,)),
            pltpu.SemaphoreType.DMA((ranks,)),
            pltpu.SemaphoreType.DMA((ranks,)),
        ],
        compiler_params=pltpu.CompilerParams(collective_id=1, has_side_effects=True),
        name="total",
    )(padded)[:count]


def body(ensemble, obs_cell, obs_value, obs_noise, obs_weight, tile_lists, batch_order):
    mem, levels, cells = ensemble.shape
    batches = obs_cell.shape[0]
    axis_size = lax.axis_size("lon")
    obs = obs_cell.shape[1] * axis_size
    slots = 32
    parts = jnp.concatenate([obs_cell.astype(f32), obs_value, obs_noise], axis=0)
    table = gathered_table(parts, axis_size)
    cell_table = table[:batches].astype(jnp.int32)
    observed = table[batches : 2 * batches]
    noise = table[2 * batches :]
    offset = lax.axis_index("lon") * CELL_DEV

    cell_table = cell_table[batch_order]
    observed = observed[batch_order]
    noise = noise[batch_order]
    weights = obs_weight[batch_order]
    lists = tile_lists[batch_order]

    owned = ((cell_table >= offset) & (cell_table < offset + CELL_DEV)).astype(f32)
    within = jnp.clip(cell_table - offset, 0, CELL_DEV - 1)

    def portion_of(inside, mine, weight):
        picked = jnp.take(ensemble, inside, axis=2)
        return jnp.sum(picked * (weight * mine[None, :])[None], axis=1)

    portions = jax.vmap(portion_of)(within, owned, weights).reshape(batches * mem, obs)
    probes = summed(portions, axis_size * lax.axis_size("lev")).reshape(batches, mem, obs)
    lists = jnp.pad(lists, ((0, 0), (0, slots - lists.shape[1])), constant_values=obs)

    call = pl.pallas_call(
        functools.partial(
            kernel_body, batches=batches, levels=levels, mem=mem, obs=obs, cells=cells, slots=slots,
            axis_size=axis_size,
        ),
        out_shape=jax.ShapeDtypeStruct((levels, mem, cells), f32),
        in_specs=[pl.BlockSpec(memory_space=pltpu.VMEM)] * 8,
        out_specs=pl.BlockSpec(memory_space=pltpu.VMEM),
        scratch_shapes=[
            pltpu.VMEM((batches, mem, obs), f32),
            pltpu.VMEM((obs, obs), f32),
            pltpu.VMEM((obs, obs), f32),
            pltpu.VMEM((slots, cells), f32),
            pltpu.VMEM((slots, 3 * mem), bf16),
            pltpu.VMEM((mem, 3 * slots), bf16),
        ],
        compiler_params=pltpu.CompilerParams(vmem_limit_bytes=40 * 1024 * 1024),
        name="assimilate",
    )
    out = call(
        ensemble.transpose(1, 0, 2),
        probes,
        observed[:, None, :],
        noise[:, None, :],
        noise[:, :, None],
        cell_table[:, None, :],
        cell_table[:, :, None],
        lists[:, :, None],
    )
    return out.transpose(1, 0, 2)


def solution(mesh):
    return jax.shard_map(
        body,
        mesh=mesh,
        in_specs=(
            P(None, "lev", "lon"),
            P(None, "lon"),
            P(None, "lon"),
            P(None, "lon"),
            P(None, "lev", None),
            P(None, "lon"),
            P(),
        ),
        out_specs=P(None, "lev", "lon"),
        check_vma=False,
    )
```

```python
import functools

import jax
import jax.numpy as jnp
from jax import lax
from jax.experimental import pallas as pl
from jax.experimental.pallas import tpu as pltpu
from jax.sharding import PartitionSpec as P

LON_DEV = 16
CELL_DEV = 1024
PANEL = 16

highest = lax.Precision.HIGHEST
f32 = jnp.float32
bf16 = jnp.bfloat16


def split(x):
    high = x.astype(bf16)
    low = (x - high.astype(f32)).astype(bf16)
    return high, low


def dot(a, b):
    return jnp.dot(a, b, preferred_element_type=f32)


def tapered_weight(row_a, col_a, row_c, col_c, circle):
    e = jnp.abs(col_a - col_c)
    e = jnp.minimum(e, circle - e)
    d = row_a - row_c
    return jnp.exp((e * e + d * d) * (-2.0 / (LON_DEV * LON_DEV)))


def eliminate(a_ref, b_ref, noise_root, mem, obs, width, beside):
    lane = lax.broadcasted_iota(jnp.int32, (1, obs), 1)
    sample = lax.broadcasted_iota(jnp.int32, (1, width), 1) < mem
    for start in range(0, obs, PANEL):
        spot = [[None] * PANEL for _ in range(PANEL)]
        for i in range(PANEL):
            for s in range(i + 1):
                spot[i][s] = jnp.broadcast_to(
                    a_ref[start + i : start + i + 1, start + s : start + s + 1], (1, obs)
                )
        in_panel = (lane >= start) & (lane < start + PANEL)
        rows = []
        sides = []
        for i in range(PANEL):
            row = a_ref[start + i : start + i + 1, :]
            rows.append(jnp.where(in_panel, jnp.where(lane == start + i, 1.0, 0.0), row))
            sides.append(b_ref[start + i : start + i + 1, :])
        scaled_rows = []
        scaled_sides = []
        for r in range(PANEL):
            pivot = spot[r][r]
            inverse_root = lax.rsqrt(pivot)
            inverse = inverse_root * inverse_root
            root = pivot * inverse_root
            added = jnp.where(sample, noise_root[start + r], 0.0)
            factor = 1.0 / (root + added)
            below = [spot[i][r] * inverse for i in range(r + 1, PANEL)]
            for n, i in enumerate(range(r + 1, PANEL)):
                for s in range(r + 1, i + 1):
                    spot[i][s] = spot[i][s] - below[n] * spot[s][r]
            solved = sides[r] * factor
            passing = solved * root
            for n, i in enumerate(range(r + 1, PANEL)):
                rows[i] = rows[i] - below[n] * rows[r]
                sides[i] = sides[i] - below[n] * passing
            scaled_rows.append(rows[r] * inverse)
            scaled_sides.append(solved * inverse_root)
            a_ref[start + r : start + r + 1, :] = jnp.where(
                lane < start + PANEL, rows[r] * inverse_root, 0.0
            )
            b_ref[start + r : start + r + 1, :] = solved
        beside(start // PANEL, obs // PANEL)
        after = start + PANEL
        if after < obs:
            u_high, u_low = split(jnp.concatenate(rows, axis=0))
            high, low = split(jnp.concatenate(
                [jnp.concatenate(scaled_rows, axis=0), jnp.concatenate(scaled_sides, axis=0)], axis=1
            ))
            upper = jnp.concatenate([u_high.astype(f32), u_high.astype(f32), u_low.astype(f32)], axis=0)
            left = upper.T.astype(bf16)[after:, :]
            change = dot(left, jnp.concatenate([high, low, high], axis=0))
            a_ref[after:, :] = jnp.where(in_panel, 0.0, a_ref[after:, :]) - change[:, :obs]
            b_ref[after:, :] = b_ref[after:, :] - change[:, obs:]


def kernel_body(
    order_ref, x_ref, landed_ref, table_ref, list_ref, out_ref,
    state, natural, probes, a_ref, b_ref, weight_ref, left_ref, gains_ref, rows_ref, noise_cols, cell_cols,
    list_cols, sem_in, sem_out, *, batches, levels, mem, obs, cells, slots, axis_size, own_max,
):
    def fetch(level):
        return pltpu.make_async_copy(x_ref.at[:, level, :], state.at[level], sem_in.at[level])

    def deliver(level):
        return pltpu.make_async_copy(state.at[level], out_ref.at[:, level, :], sem_out.at[level])

    for level in range(levels):
        fetch(level).start()
    tile = lax.axis_index("lon")
    circle = float(LON_DEV * axis_size)
    scale = 1.0 / (mem - 1)
    cell = lax.broadcasted_iota(jnp.int32, (1, cells), 1)
    here_row = (cell // LON_DEV).astype(f32)
    here_col = (tile * LON_DEV + cell % LON_DEV).astype(f32)
    lanes = lax.broadcasted_iota(jnp.int32, (obs, obs), 1)
    subs = lax.broadcasted_iota(jnp.int32, (obs, obs), 0)
    table = table_ref[...]
    rows = table.T
    rows_ref[...] = rows
    count = axis_size * own_max
    spot = lax.broadcasted_iota(jnp.int32, (count, obs), 0).astype(f32)
    listed_rows = jnp.concatenate(
        [list_ref[...].astype(f32), jnp.full((batches, obs - list_ref.shape[1]), float(obs), f32)], axis=1
    )
    listed_rows = jnp.concatenate([listed_rows, jnp.zeros((obs - batches, obs), f32)], axis=0).T
    parts = landed_ref.shape[1]
    share = -(-batches // parts)
    for b in range(batches):
        cell_row = rows[b : b + 1, :].astype(jnp.int32)
        tile_row = cell_row // CELL_DEV
        cell_col = jnp.broadcast_to(table[:, b : b + 1], (obs, obs))
        tile_col = cell_col.astype(jnp.int32) // CELL_DEV
        earlier = (tile_col == tile_row) & (subs < lanes)
        rank = jnp.sum(jnp.where(earlier, 1.0, 0.0), axis=0, keepdims=True)
        slot = tile_row.astype(f32) * own_max + rank
        found = jnp.where(spot == slot, 1.0, 0.0).astype(bf16)
        first = b % share * mem
        slab = landed_ref[:, b // share, :, first : first + mem].reshape(count, mem)
        high, low = split(slab)
        left = jnp.concatenate([high.astype(f32), low.astype(f32)], axis=0).T.astype(bf16)
        natural[b] = dot(left, jnp.concatenate([found, found], axis=0))
        noise_cols[b] = jnp.sqrt(jnp.broadcast_to(table[:, 2 * batches + b : 2 * batches + b + 1], (obs, obs)))
        cell_cols[b] = cell_col
        list_cols[b] = jnp.broadcast_to(listed_rows[:slots, b : b + 1], (slots, obs))

    def arrange(k, carry):
        probes[k] = natural[order_ref[k]]
        return carry

    lax.fori_loop(0, batches, arrange, 0)

    def place_of(cells_now):
        cells_now = cells_now.astype(jnp.int32)
        its_tile = cells_now // CELL_DEV
        within = cells_now - its_tile * CELL_DEV
        row = within // LON_DEV
        col = its_tile * LON_DEV + within - row * LON_DEV
        return row.astype(f32), col.astype(f32), its_tile.astype(f32)

    def spread_piece(level, start, width):
        piece = pl.ds(start, width)
        block = state[level, :, piece]
        high, low = split(block)
        crossed = dot(left_ref[...], jnp.concatenate([high, low, high], axis=0))
        high, low = split(crossed * weight_ref[:, piece])
        state[level, :, piece] = block + dot(gains_ref[...], jnp.concatenate([high, low, high], axis=0))

    def beside(step, steps):
        halves = 2 * levels
        for piece in range(step * halves // steps, (step + 1) * halves // steps):
            spread_piece(piece // 2, piece % 2 * (cells // 2), cells // 2)

    def turn(k, carry):
        block = order_ref[k]
        now = probes[k]
        centre = jnp.mean(now, axis=0, keepdims=True)
        spread = now - centre
        innovation = rows_ref[pl.ds(batches + block, 1), :] - centre
        padded = jnp.concatenate(
            [spread, innovation, jnp.zeros((obs - mem - 1, obs), f32)], axis=0
        )
        sides = padded.T
        noise_row = rows_ref[pl.ds(2 * batches + block, 1), :]
        covariance = jnp.dot(sides[:, :mem], spread, precision=highest, preferred_element_type=f32) * scale
        a_ref[...] = covariance + jnp.where(lanes == subs, noise_row, 0.0)
        b_ref[...] = sides
        root_col = noise_cols[block]
        roots = [root_col[j : j + 1, :] for j in range(obs)]
        eliminate(a_ref, b_ref, roots, mem, obs, obs, beside)
        joined = lax.dot_general(
            a_ref[...], b_ref[...], (((0,), (0,)), ((), ())), precision=highest, preferred_element_type=f32
        )
        gain_t = joined[:, mem : mem + 1] - joined
        gain = gain_t.T[:mem, :]

        s_high, s_low = split(spread)
        stacked = jnp.concatenate([s_high.astype(f32), s_high.astype(f32), s_low.astype(f32)], axis=0)
        left = stacked.T.astype(bf16)
        g_high, g_low = split(gain)
        gains = jnp.concatenate([g_high, g_high, g_low], axis=1)

        from_row, from_col, from_tile = place_of(cell_cols[block])

        def renew(b, carry):
            @pl.when(2 * b + 1 > k)
            def _():
                upcoming = jnp.concatenate([probes[2 * b], probes[2 * b + 1]], axis=1)
                high, low = split(upcoming)
                crossed = dot(left, jnp.concatenate([high, low, high], axis=0))
                weights = []
                for u in range(2):
                    target_row, target_col, target_tile = place_of(
                        rows_ref[pl.ds(order_ref[2 * b + u], 1), :]
                    )
                    weight = tapered_weight(from_row, from_col, target_row, target_col, circle)
                    apart = jnp.abs(from_tile - target_tile)
                    near = (apart < 1.5) | (apart > axis_size - 1.5)
                    weights.append(jnp.where(near, weight * scale, 0.0))
                tapered = crossed * jnp.concatenate(weights, axis=1)
                high, low = split(tapered)
                upcoming = upcoming + dot(gains, jnp.concatenate([high, low, high], axis=0))
                probes[2 * b] = upcoming[:, :obs]
                probes[2 * b + 1] = upcoming[:, obs:]

            return carry

        for b in range(batches // 2):
            renew(b, 0)

        listed = list_cols[block]
        chosen = lanes[:slots].astype(f32) == listed
        select = chosen.astype(bf16)
        pick_row, pick_col, _ = place_of(rows_ref[pl.ds(block, 1), :])
        list_row = jnp.sum(jnp.where(chosen, pick_row, 0.0), axis=1, keepdims=True)
        list_col = jnp.sum(jnp.where(chosen, pick_col, 0.0), axis=1, keepdims=True)
        usable = jnp.where(listed[:, :1] < obs, scale, 0.0)
        weight = tapered_weight(list_row, list_col, here_row, here_col, circle) * usable
        left_listed = dot(select, left).astype(bf16)
        gt_high, gt_low = split(gain_t)
        gt_high = dot(select, gt_high)
        gt_low = dot(select, gt_low)
        gains_listed = jnp.concatenate([gt_high, gt_high, gt_low, jnp.zeros((obs - 3 * slots, obs), f32)], axis=0)
        gains_listed = gains_listed.T[:mem, : 3 * slots].astype(bf16)

        weight_ref[...] = weight
        left_ref[...] = left_listed
        gains_ref[...] = gains_listed
        return carry

    weight_ref[...] = jnp.zeros(weight_ref.shape, f32)
    left_ref[...] = jnp.zeros(left_ref.shape, bf16)
    gains_ref[...] = jnp.zeros(gains_ref.shape, bf16)
    for level in range(levels):
        fetch(level).wait()
    lax.fori_loop(0, batches, turn, 0)

    def last(level, carry):
        spread_piece(level, 0, cells)
        deliver(level).start()
        return carry

    lax.fori_loop(0, levels, last, 0)
    for level in range(levels):
        deliver(level).wait()


def gather_kernel(
    x_ref, cell_ref, value_ref, noise_ref, weight_ref, landed, table_ref,
    x_in, mine, tables, packed, partial, total, x_sem,
    table_send, table_recv, pair_send, pair_recv, send_sem, recv_sem, pass_send, pass_recv,
    *, ranks, cores, batches, mem, levels, cells, obs, own_max,
):
    lon, lev = lax.axis_index("lon"), lax.axis_index("lev")
    mesh_id = pl.DeviceIdType.MESH
    fetch = pltpu.make_async_copy(x_ref, x_in, x_sem)
    fetch.start()
    own = cell_ref.shape[0]
    depth = mine.shape[0]
    row = jnp.concatenate(
        [cell_ref[...].astype(f32), value_ref[...], noise_ref[...], jnp.zeros((own, 128 - 3 * batches), f32)], axis=1
    )
    if own < depth:
        row = jnp.concatenate([row, jnp.zeros((depth - own, 128), f32)], axis=0)
    mine[...] = row

    def chip(d):
        return lax.rem(lon + d, ranks), lev

    def core(d):
        return lon, lax.rem(lev + d, cores)

    barrier = pltpu.get_barrier_semaphore()

    def announce(d, carry):
        pl.semaphore_signal(barrier, inc=1, device_id=chip(d), device_id_type=mesh_id)
        return carry

    lax.fori_loop(1, ranks, announce, 0)
    for d in range(1, cores):
        pl.semaphore_signal(barrier, inc=1, device_id=core(d), device_id_type=mesh_id)
    pl.semaphore_wait(barrier, ranks + cores - 2)

    def table_to(d):
        return pltpu.make_async_remote_copy(
            src_ref=mine, dst_ref=tables.at[lon], send_sem=table_send.at[d], recv_sem=table_recv.at[d],
            device_id=chip(d), device_id_type=mesh_id,
        )

    def start_table(d, carry):
        table_to(d).start()
        return carry

    def wait_table(d, carry):
        table_to(d).wait()
        return carry

    lax.fori_loop(1, ranks, start_table, 0)
    tables[lon] = row
    lax.fori_loop(1, ranks, wait_table, 0)
    if own == depth:
        table = tables[...].reshape(obs, 128)
    else:
        table = jnp.concatenate([tables[t, :own, :] for t in range(ranks)], axis=0)
    table_ref[...] = table

    lane = lax.broadcasted_iota(jnp.int32, (obs, 128), 1)
    sub = lax.broadcasted_iota(jnp.int32, (obs, 128), 0)
    cell = jnp.where(lane < batches, table, -1.0).astype(jnp.int32)
    within = cell - lon * cells
    owned = (within >= 0) & (within < cells)
    before = jnp.where(lax.broadcasted_iota(jnp.int32, (obs, obs), 1) < lax.broadcasted_iota(jnp.int32, (obs, obs), 0), 1.0, 0.0)
    rank = dot(before.astype(bf16), jnp.where(owned, 1.0, 0.0).astype(bf16))
    code = jnp.where(owned, rank, -1.0)
    within = jnp.where(owned, within, 0)
    upper = within // LON_DEV
    lower = within - upper * LON_DEV
    deep = lax.broadcasted_iota(jnp.int32, (128, 128), 0)
    wide = lax.broadcasted_iota(jnp.int32, (128, 128), 1)
    spread_out = jnp.where((wide // own_max == deep) & (deep < batches), 1.0, 0.0).astype(bf16)
    wide_code = dot(code.astype(bf16), spread_out)
    wide_upper = dot(upper.astype(f32).astype(bf16), spread_out)
    wide_lower = dot(lower.astype(f32).astype(bf16), spread_out)
    slot = (lane - lane // own_max * own_max).astype(f32)
    taken = (wide_code == slot) & (lane < batches * own_max)
    chosen = jnp.where(taken, 1.0, 0.0)
    column = jnp.sum(jnp.where(taken, wide_upper * LON_DEV + wide_lower, 0.0), axis=0, keepdims=True)
    weighed = jnp.dot(
        weight_ref[...].reshape(batches * levels, obs), chosen, precision=highest, preferred_element_type=f32
    )
    block_of = lax.broadcasted_iota(jnp.int32, (levels, 128), 1) // own_max
    weight = jnp.zeros((levels, 128), f32)
    for b in range(batches):
        weight = jnp.where(block_of == b, weighed[b * levels : (b + 1) * levels, :], weight)
    at = lax.broadcasted_iota(jnp.int32, (cells, 128), 0).astype(f32)
    hot = jnp.where(at == column, 1.0, 0.0).astype(bf16)
    fetch.wait()
    pieces = []
    group = 16
    for m in range(0, mem, group):
        part = x_in[m : m + group].reshape(group * levels, cells)
        high, low = split(part)
        picked = (dot(high, hot) + dot(low, hot)).reshape(group, levels, 128)
        pieces.append(jnp.sum(picked * weight[None], axis=1))
    portion = jnp.concatenate(pieces + [jnp.zeros((128 - mem, 128), f32)], axis=0).T
    share = -(-batches // cores)
    width = packed.shape[2]
    for h in range(cores):
        line = [portion[b * own_max : (b + 1) * own_max, :mem] for b in range(h * share, min((h + 1) * share, batches))]
        gap = width - len(line) * mem
        if gap:
            line.append(jnp.zeros((own_max, gap), f32))
        packed[h] = jnp.concatenate(line, axis=1)

    def pair_to(d):
        return pltpu.make_async_remote_copy(
            src_ref=packed.at[lax.rem(lev + d, cores)], dst_ref=partial.at[d], send_sem=pair_send.at[d],
            recv_sem=pair_recv.at[d], device_id=core(d), device_id_type=mesh_id,
        )

    for d in range(1, cores):
        pair_to(d).start()
    sum_now = packed[lev]
    for d in range(1, cores):
        pair_to(d).wait()
        sum_now = sum_now + partial[d]
    total[...] = sum_now

    def send_to(d):
        return pltpu.make_async_remote_copy(
            src_ref=total, dst_ref=landed.at[lon, lev], send_sem=send_sem.at[d], recv_sem=recv_sem.at[d],
            device_id=chip(d), device_id_type=mesh_id,
        )

    def give_to(d):
        return pltpu.make_async_remote_copy(
            src_ref=total, dst_ref=landed.at[lon, lev], send_sem=pass_send.at[d, 0], recv_sem=pass_recv.at[d, 0],
            device_id=core(d), device_id_type=mesh_id,
        )

    def pass_on(d, e):
        source = lax.rem(lon - d + ranks, ranks)
        return pltpu.make_async_remote_copy(
            src_ref=landed.at[source, lev], dst_ref=landed.at[source, lev], send_sem=pass_send.at[e, d],
            recv_sem=pass_recv.at[e, d], device_id=core(e), device_id_type=mesh_id,
        )

    def start_send(d, carry):
        send_to(d).start()
        return carry

    def relay(d, carry):
        send_to(d).wait()
        for e in range(1, cores):
            pass_on(d, e).start()
        return carry

    def wait_relay(d, carry):
        for e in range(1, cores):
            pass_on(d, e).wait()
        return carry

    lax.fori_loop(1, ranks, start_send, 0)
    for d in range(1, cores):
        give_to(d).start()
    landed[lon, lev] = sum_now
    lax.fori_loop(1, ranks, relay, 0)
    for d in range(1, cores):
        give_to(d).wait()
    lax.fori_loop(1, ranks, wait_relay, 0)


def body(ensemble, obs_cell, obs_value, obs_noise, obs_weight, tile_lists, batch_order):
    mem, levels, cells = ensemble.shape
    batches, own = obs_cell.shape
    ranks, cores = lax.axis_size("lon"), lax.axis_size("lev")
    obs = own * ranks
    own_max = 8
    slots = -(-tile_lists.shape[1] // 16) * 16
    width = -(-(-(-batches // cores) * mem) // 128) * 128
    depth = -(-own // 8) * 8
    vmem = pl.BlockSpec(memory_space=pltpu.VMEM)
    hbm = pl.BlockSpec(memory_space=pl.ANY)
    dma = pltpu.SemaphoreType.DMA
    landed, table = pl.pallas_call(
        functools.partial(
            gather_kernel, ranks=ranks, cores=cores, batches=batches, mem=mem, levels=levels, cells=cells,
            obs=obs, own_max=own_max,
        ),
        out_shape=[
            jax.ShapeDtypeStruct((ranks, cores, own_max, width), f32), jax.ShapeDtypeStruct((obs, 128), f32)
        ],
        in_specs=[hbm] + [vmem] * 4,
        out_specs=[vmem, vmem],
        scratch_shapes=[
            pltpu.VMEM((mem, levels, cells), f32),
            pltpu.VMEM((depth, 128), f32),
            pltpu.VMEM((ranks, depth, 128), f32),
            pltpu.VMEM((cores, own_max, width), f32),
            pltpu.VMEM((cores, own_max, width), f32),
            pltpu.VMEM((own_max, width), f32),
            dma(()), dma((ranks,)), dma((ranks,)), dma((cores,)), dma((cores,)), dma((ranks,)), dma((ranks,)),
            dma((cores, ranks)), dma((cores, ranks)),
        ],
        compiler_params=pltpu.CompilerParams(
            collective_id=0, has_side_effects=True, vmem_limit_bytes=40 * 1024 * 1024
        ),
        name="gather",
    )(ensemble, obs_cell.T, obs_value.T, obs_noise.T, obs_weight)

    return pl.pallas_call(
        functools.partial(
            kernel_body, batches=batches, levels=levels, mem=mem, obs=obs, cells=cells, slots=slots,
            axis_size=ranks, own_max=own_max,
        ),
        out_shape=jax.ShapeDtypeStruct((mem, levels, cells), f32),
        in_specs=[pl.BlockSpec(memory_space=pltpu.SMEM), hbm, vmem, vmem, vmem],
        out_specs=hbm,
        scratch_shapes=[
            pltpu.VMEM((levels, mem, cells), f32),
            pltpu.VMEM((batches, mem, obs), f32),
            pltpu.VMEM((batches, mem, obs), f32),
            pltpu.VMEM((obs, obs), f32),
            pltpu.VMEM((obs, obs), f32),
            pltpu.VMEM((slots, cells), f32),
            pltpu.VMEM((slots, 3 * mem), bf16),
            pltpu.VMEM((mem, 3 * slots), bf16),
            pltpu.VMEM((128, obs), f32),
            pltpu.VMEM((batches, obs, obs), f32),
            pltpu.VMEM((batches, obs, obs), f32),
            pltpu.VMEM((batches, slots, obs), f32),
            dma((levels,)),
            dma((levels,)),
        ],
        compiler_params=pltpu.CompilerParams(vmem_limit_bytes=40 * 1024 * 1024),
        name="assimilate",
    )(batch_order, ensemble, landed, table, tile_lists)


def solution(mesh):
    return jax.shard_map(
        body,
        mesh=mesh,
        in_specs=(
            P(None, "lev", "lon"),
            P(None, "lon"),
            P(None, "lon"),
            P(None, "lon"),
            P(None, "lev", None),
            P(None, "lon"),
            P(),
        ),
        out_specs=P(None, "lev", "lon"),
        check_vma=False,
    )
```

```python
import functools

import jax
import jax.numpy as jnp
from jax import lax
from jax.experimental import pallas as pl
from jax.experimental.pallas import tpu as pltpu
from jax.sharding import PartitionSpec as P

LON_DEV = 16
CELL_DEV = 1024
PANEL = 16
GROUP = 2

highest = lax.Precision.HIGHEST
f32 = jnp.float32
bf16 = jnp.bfloat16


def split(x):
    high = x.astype(bf16)
    low = (x - high.astype(f32)).astype(bf16)
    return high, low


def dot(a, b):
    return jnp.dot(a, b, preferred_element_type=f32)


def tapered_weight(row_a, col_a, row_c, col_c, circle):
    e = jnp.abs(col_a - col_c)
    e = jnp.minimum(e, circle - e)
    d = row_a - row_c
    return jnp.exp((e * e + d * d) * (-2.0 / (LON_DEV * LON_DEV)))


def eliminate(a_ref, b_ref, noise_root, mem, obs, width, beside):
    lane = lax.broadcasted_iota(jnp.int32, (1, obs), 1)
    sample = lax.broadcasted_iota(jnp.int32, (1, width), 1) < mem
    for start in range(0, obs, PANEL):
        spot = [[None] * PANEL for _ in range(PANEL)]
        for i in range(PANEL):
            for s in range(i + 1):
                spot[i][s] = jnp.broadcast_to(
                    a_ref[start + i : start + i + 1, start + s : start + s + 1], (1, obs)
                )
        in_panel = (lane >= start) & (lane < start + PANEL)
        rows = []
        sides = []
        for i in range(PANEL):
            row = a_ref[start + i : start + i + 1, :]
            rows.append(jnp.where(in_panel, jnp.where(lane == start + i, 1.0, 0.0), row))
            sides.append(b_ref[start + i : start + i + 1, :])
        scaled_rows = []
        scaled_sides = []
        for r in range(PANEL):
            pivot = spot[r][r]
            inverse_root = lax.rsqrt(pivot)
            inverse = inverse_root * inverse_root
            root = pivot * inverse_root
            added = jnp.where(sample, noise_root[start + r], 0.0)
            factor = 1.0 / (root + added)
            below = [spot[i][r] * inverse for i in range(r + 1, PANEL)]
            for n, i in enumerate(range(r + 1, PANEL)):
                for s in range(r + 1, i + 1):
                    spot[i][s] = spot[i][s] - below[n] * spot[s][r]
            solved = sides[r] * factor
            passing = solved * root
            for n, i in enumerate(range(r + 1, PANEL)):
                rows[i] = rows[i] - below[n] * rows[r]
                sides[i] = sides[i] - below[n] * passing
            scaled_rows.append(rows[r] * inverse)
            scaled_sides.append(solved * inverse_root)
            a_ref[start + r : start + r + 1, :] = jnp.where(
                lane < start + PANEL, rows[r] * inverse_root, 0.0
            )
            b_ref[start + r : start + r + 1, :] = solved
        beside(start // PANEL, obs // PANEL)
        after = start + PANEL
        if after < obs:
            u_high, u_low = split(jnp.concatenate(rows, axis=0))
            high, low = split(jnp.concatenate(
                [jnp.concatenate(scaled_rows, axis=0), jnp.concatenate(scaled_sides, axis=0)], axis=1
            ))
            upper = jnp.concatenate([u_high.astype(f32), u_high.astype(f32), u_low.astype(f32)], axis=0)
            left = upper.T.astype(bf16)[after:, :]
            change = dot(left, jnp.concatenate([high, low, high], axis=0))
            a_ref[after:, :] = jnp.where(in_panel, 0.0, a_ref[after:, :]) - change[:, :obs]
            b_ref[after:, :] = b_ref[after:, :] - change[:, obs:]


def kernel_body(
    order_ref, x_ref, landed_ref, table_ref, list_hbm, out_ref,
    state, natural, probes, a_ref, b_ref, weight_ref, left_ref, gains_ref, rows_ref, noise_cols, cell_cols,
    list_cols, list_ref, sem_list, sem_in, sem_out, *, batches, levels, mem, obs, cells, slots, axis_size, own_max,
):
    def fetch(level):
        return pltpu.make_async_copy(x_ref.at[:, level, :], state.at[level], sem_in.at[level])

    def deliver(level):
        return pltpu.make_async_copy(state.at[level], out_ref.at[:, level, :], sem_out.at[level])

    list_copy = pltpu.make_async_copy(list_hbm, list_ref, sem_list)
    list_copy.start()
    for level in range(levels):
        fetch(level).start()
    tile = lax.axis_index("lon")
    circle = float(LON_DEV * axis_size)
    scale = 1.0 / (mem - 1)
    cell = lax.broadcasted_iota(jnp.int32, (1, cells), 1)
    here_row = (cell // LON_DEV).astype(f32)
    here_col = (tile * LON_DEV + cell % LON_DEV).astype(f32)
    lanes = lax.broadcasted_iota(jnp.int32, (obs, obs), 1)
    subs = lax.broadcasted_iota(jnp.int32, (obs, obs), 0)
    table = table_ref[...]
    rows = table.T
    rows_ref[...] = rows
    count = axis_size * own_max
    spot = lax.broadcasted_iota(jnp.int32, (count, obs), 0).astype(f32)
    list_copy.wait()
    listed_rows = jnp.concatenate(
        [list_ref[...].astype(f32), jnp.full((batches, obs - list_ref.shape[1]), float(obs), f32)], axis=1
    )
    listed_rows = jnp.concatenate([listed_rows, jnp.zeros((obs - batches, obs), f32)], axis=0).T
    parts = landed_ref.shape[1]
    share = -(-batches // parts)
    lane_b = lanes[:, :128]
    tile_cols = (jnp.where(lane_b < batches, table, 0.0).astype(jnp.int32) // CELL_DEV).astype(f32)
    tile_rows = tile_cols.T
    roots_all = jnp.sqrt(jnp.where((lane_b >= 2 * batches) & (lane_b < 3 * batches), table, 1.0))
    sooner = jnp.where(subs < lanes, 1.0, 0.0)
    for b in range(batches):
        tile_row = tile_rows[b : b + 1, :]
        tile_col = jnp.broadcast_to(tile_cols[:, b : b + 1], (obs, obs))
        rank = jnp.sum(jnp.where(tile_col == tile_row, sooner, 0.0), axis=0, keepdims=True)
        slot = tile_row * own_max + rank
        found = jnp.where(spot == slot, 1.0, 0.0).astype(bf16)
        first = b % share * mem
        slab = landed_ref[:, b // share, :, first : first + mem].reshape(count, mem)
        high, low = split(slab)
        left = jnp.concatenate([high.astype(f32), low.astype(f32)], axis=0).T.astype(bf16)
        natural[b] = dot(left, jnp.concatenate([found, found], axis=0))
        noise_cols[b] = jnp.broadcast_to(roots_all[:, 2 * batches + b : 2 * batches + b + 1], (obs, obs))
        cell_cols[b] = jnp.broadcast_to(table[:, b : b + 1], (obs, obs))
        list_cols[b] = jnp.broadcast_to(listed_rows[:slots, b : b + 1], (slots, obs))

    def arrange(k, carry):
        probes[k] = natural[order_ref[k]]
        return carry

    lax.fori_loop(0, batches, arrange, 0)

    def place_of(cells_now):
        cells_now = cells_now.astype(jnp.int32)
        its_tile = cells_now // CELL_DEV
        within = cells_now - its_tile * CELL_DEV
        row = within // LON_DEV
        col = its_tile * LON_DEV + within - row * LON_DEV
        return row.astype(f32), col.astype(f32), its_tile.astype(f32)

    def spread_piece(level, start, width):
        piece = pl.ds(start, width)
        block = state[level, :, piece]
        high, low = split(block)
        crossed = dot(left_ref[...], jnp.concatenate([high, low, high], axis=0))
        high, low = split(crossed * weight_ref[:, piece])
        state[level, :, piece] = block + dot(gains_ref[...], jnp.concatenate([high, low, high], axis=0))

    def beside(step, steps):
        halves = 2 * levels
        for piece in range(step * halves // steps, (step + 1) * halves // steps):
            spread_piece(piece // 2, piece % 2 * (cells // 2), cells // 2)

    def turn(k, carry):
        block = order_ref[k]
        now = probes[k]
        centre = jnp.mean(now, axis=0, keepdims=True)
        spread = now - centre
        innovation = rows_ref[pl.ds(batches + block, 1), :] - centre
        padded = jnp.concatenate(
            [spread, innovation, jnp.zeros((obs - mem - 1, obs), f32)], axis=0
        )
        sides = padded.T
        noise_row = rows_ref[pl.ds(2 * batches + block, 1), :]
        s_high, s_low = split(spread)
        stacked = jnp.concatenate([s_high.astype(f32), s_high.astype(f32), s_low.astype(f32)], axis=0)
        left = stacked.T.astype(bf16)
        covariance = dot(left, jnp.concatenate([s_high, s_low, s_high], axis=0)) * scale
        a_ref[...] = covariance + jnp.where(lanes == subs, noise_row, 0.0)
        b_ref[...] = sides
        root_col = noise_cols[block]
        roots = [root_col[j : j + 1, :] for j in range(obs)]
        eliminate(a_ref, b_ref, roots, mem, obs, obs, beside)
        f_high, f_low = split(a_ref[...].T)
        b_high, b_low = split(b_ref[...])
        joined = dot(
            jnp.concatenate([f_high, f_high, f_low], axis=1), jnp.concatenate([b_high, b_low, b_high], axis=0)
        )
        gain_t = joined[:, mem : mem + 1] - joined
        gain = gain_t.T[:mem, :]

        g_high, g_low = split(gain)
        gains = jnp.concatenate([g_high, g_high, g_low], axis=1)

        from_row, from_col, from_tile = place_of(cell_cols[block])

        def renew(first):
            @pl.when(first + GROUP - 1 > k)
            def _():
                members = range(first, first + GROUP)
                upcoming = jnp.concatenate([probes[j] for j in members], axis=1)
                high, low = split(upcoming)
                crossed = dot(left, jnp.concatenate([high, low, high], axis=0))
                weights = []
                for j in members:
                    target_row, target_col, target_tile = place_of(rows_ref[pl.ds(order_ref[j], 1), :])
                    weight = tapered_weight(from_row, from_col, target_row, target_col, circle)
                    apart = jnp.abs(from_tile - target_tile)
                    near = (apart < 1.5) | (apart > axis_size - 1.5)
                    weights.append(jnp.where(near, weight * scale, 0.0))
                high, low = split(crossed * jnp.concatenate(weights, axis=1))
                upcoming = upcoming + dot(gains, jnp.concatenate([high, low, high], axis=0))
                for n, j in enumerate(members):
                    probes[j] = upcoming[:, n * obs : (n + 1) * obs]

        for first in range(0, batches, GROUP):
            renew(first)

        listed = list_cols[block]
        chosen = lanes[:slots].astype(f32) == listed
        select = chosen.astype(bf16)
        pick_row, pick_col, _ = place_of(rows_ref[pl.ds(block, 1), :])
        list_row = jnp.sum(jnp.where(chosen, pick_row, 0.0), axis=1, keepdims=True)
        list_col = jnp.sum(jnp.where(chosen, pick_col, 0.0), axis=1, keepdims=True)
        usable = jnp.where(listed[:, :1] < obs, scale, 0.0)
        weight = tapered_weight(list_row, list_col, here_row, here_col, circle) * usable
        left_listed = dot(select, left).astype(bf16)
        gt_high, gt_low = split(gain_t)
        gt_high = dot(select, gt_high)
        gt_low = dot(select, gt_low)
        gains_listed = jnp.concatenate([gt_high, gt_high, gt_low, jnp.zeros((obs - 3 * slots, obs), f32)], axis=0)
        gains_listed = gains_listed.T[:mem, : 3 * slots].astype(bf16)

        weight_ref[...] = weight
        left_ref[...] = left_listed
        gains_ref[...] = gains_listed
        return carry

    weight_ref[...] = jnp.zeros(weight_ref.shape, f32)
    left_ref[...] = jnp.zeros(left_ref.shape, bf16)
    gains_ref[...] = jnp.zeros(gains_ref.shape, bf16)
    for level in range(levels):
        fetch(level).wait()
    lax.fori_loop(0, batches, turn, 0)

    def last(level, carry):
        spread_piece(level, 0, cells)
        deliver(level).start()
        return carry

    lax.fori_loop(0, levels, last, 0)
    for level in range(levels):
        deliver(level).wait()


def gather_kernel(
    x_ref, cell_hbm, value_hbm, noise_hbm, weight_hbm, landed, table_ref,
    x_in, cell_ref, value_ref, noise_ref, weight_ref, small_sem, mine, tables, packed, partial, total, x_sem,
    table_send, table_recv, pair_send, pair_recv, send_sem, recv_sem, pass_send, pass_recv,
    *, ranks, cores, batches, mem, levels, cells, obs, own_max,
):
    lon, lev = lax.axis_index("lon"), lax.axis_index("lev")
    mesh_id = pl.DeviceIdType.MESH
    fetch = pltpu.make_async_copy(x_ref, x_in, x_sem)
    small = [
        pltpu.make_async_copy(src, dst, small_sem.at[i])
        for i, (src, dst) in enumerate(
            [(cell_hbm, cell_ref), (value_hbm, value_ref), (noise_hbm, noise_ref), (weight_hbm, weight_ref)]
        )
    ]
    for copy in small:
        copy.start()
    fetch.start()
    for copy in small[:3]:
        copy.wait()
    own = cell_ref.shape[0]
    depth = mine.shape[0]
    row = jnp.concatenate(
        [cell_ref[...].astype(f32), value_ref[...], noise_ref[...], jnp.zeros((own, 128 - 3 * batches), f32)], axis=1
    )
    if own < depth:
        row = jnp.concatenate([row, jnp.zeros((depth - own, 128), f32)], axis=0)
    mine[...] = row

    def chip(d):
        return lax.rem(lon + d, ranks), lev

    def core(d):
        return lon, lax.rem(lev + d, cores)

    barrier = pltpu.get_barrier_semaphore()

    def announce(d, carry):
        pl.semaphore_signal(barrier, inc=1, device_id=chip(d), device_id_type=mesh_id)
        return carry

    lax.fori_loop(1, ranks, announce, 0)
    for d in range(1, cores):
        pl.semaphore_signal(barrier, inc=1, device_id=core(d), device_id_type=mesh_id)
    pl.semaphore_wait(barrier, ranks + cores - 2)

    def table_to(d):
        return pltpu.make_async_remote_copy(
            src_ref=mine, dst_ref=tables.at[lon], send_sem=table_send.at[d], recv_sem=table_recv.at[d],
            device_id=chip(d), device_id_type=mesh_id,
        )

    def start_table(d, carry):
        table_to(d).start()
        return carry

    def wait_table(d, carry):
        table_to(d).wait()
        return carry

    lax.fori_loop(1, ranks, start_table, 0)
    tables[lon] = row
    lax.fori_loop(1, ranks, wait_table, 0)
    if own == depth:
        table = tables[...].reshape(obs, 128)
    else:
        table = jnp.concatenate([tables[t, :own, :] for t in range(ranks)], axis=0)
    table_ref[...] = table

    lane = lax.broadcasted_iota(jnp.int32, (obs, 128), 1)
    sub = lax.broadcasted_iota(jnp.int32, (obs, 128), 0)
    cell = jnp.where(lane < batches, table, -1.0).astype(jnp.int32)
    within = cell - lon * cells
    owned = (within >= 0) & (within < cells)
    before = jnp.where(lax.broadcasted_iota(jnp.int32, (obs, obs), 1) < lax.broadcasted_iota(jnp.int32, (obs, obs), 0), 1.0, 0.0)
    rank = dot(before.astype(bf16), jnp.where(owned, 1.0, 0.0).astype(bf16))
    code = jnp.where(owned, rank, -1.0)
    within = jnp.where(owned, within, 0)
    upper = within // LON_DEV
    lower = within - upper * LON_DEV
    deep = lax.broadcasted_iota(jnp.int32, (128, 128), 0)
    wide = lax.broadcasted_iota(jnp.int32, (128, 128), 1)
    spread_out = jnp.where((wide // own_max == deep) & (deep < batches), 1.0, 0.0).astype(bf16)
    wide_code = dot(code.astype(bf16), spread_out)
    wide_upper = dot(upper.astype(f32).astype(bf16), spread_out)
    wide_lower = dot(lower.astype(f32).astype(bf16), spread_out)
    slot = (lane - lane // own_max * own_max).astype(f32)
    taken = (wide_code == slot) & (lane < batches * own_max)
    chosen = jnp.where(taken, 1.0, 0.0)
    column = jnp.sum(jnp.where(taken, wide_upper * LON_DEV + wide_lower, 0.0), axis=0, keepdims=True)
    small[3].wait()
    weighed = jnp.dot(
        weight_ref[...].reshape(batches * levels, obs), chosen, precision=highest, preferred_element_type=f32
    )
    block_of = lax.broadcasted_iota(jnp.int32, (levels, 128), 1) // own_max
    weight = jnp.zeros((levels, 128), f32)
    for b in range(batches):
        weight = jnp.where(block_of == b, weighed[b * levels : (b + 1) * levels, :], weight)
    at = lax.broadcasted_iota(jnp.int32, (cells, 128), 0).astype(f32)
    hot = jnp.where(at == column, 1.0, 0.0).astype(bf16)
    fetch.wait()
    pieces = []
    group = 16
    for m in range(0, mem, group):
        part = x_in[m : m + group].reshape(group * levels, cells)
        high, low = split(part)
        picked = (dot(high, hot) + dot(low, hot)).reshape(group, levels, 128)
        pieces.append(jnp.sum(picked * weight[None], axis=1))
    portion = jnp.concatenate(pieces + [jnp.zeros((128 - mem, 128), f32)], axis=0).T
    share = -(-batches // cores)
    width = packed.shape[2]
    for h in range(cores):
        line = [portion[b * own_max : (b + 1) * own_max, :mem] for b in range(h * share, min((h + 1) * share, batches))]
        gap = width - len(line) * mem
        if gap:
            line.append(jnp.zeros((own_max, gap), f32))
        packed[h] = jnp.concatenate(line, axis=1)

    def pair_to(d):
        return pltpu.make_async_remote_copy(
            src_ref=packed.at[lax.rem(lev + d, cores)], dst_ref=partial.at[d], send_sem=pair_send.at[d],
            recv_sem=pair_recv.at[d], device_id=core(d), device_id_type=mesh_id,
        )

    for d in range(1, cores):
        pair_to(d).start()
    sum_now = packed[lev]
    for d in range(1, cores):
        pair_to(d).wait()
        sum_now = sum_now + partial[d]
    total[...] = sum_now

    def send_to(d):
        return pltpu.make_async_remote_copy(
            src_ref=total, dst_ref=landed.at[lon, lev], send_sem=send_sem.at[d], recv_sem=recv_sem.at[d],
            device_id=chip(d), device_id_type=mesh_id,
        )

    def give_to(d):
        return pltpu.make_async_remote_copy(
            src_ref=total, dst_ref=landed.at[lon, lev], send_sem=pass_send.at[d, 0], recv_sem=pass_recv.at[d, 0],
            device_id=core(d), device_id_type=mesh_id,
        )

    def pass_on(d, e):
        source = lax.rem(lon - d + ranks, ranks)
        return pltpu.make_async_remote_copy(
            src_ref=landed.at[source, lev], dst_ref=landed.at[source, lev], send_sem=pass_send.at[e, d],
            recv_sem=pass_recv.at[e, d], device_id=core(e), device_id_type=mesh_id,
        )

    def start_send(d, carry):
        send_to(d).start()
        return carry

    def relay(d, carry):
        send_to(d).wait()
        for e in range(1, cores):
            pass_on(d, e).start()
        return carry

    def wait_relay(d, carry):
        for e in range(1, cores):
            pass_on(d, e).wait()
        return carry

    lax.fori_loop(1, ranks, start_send, 0)
    for d in range(1, cores):
        give_to(d).start()
    landed[lon, lev] = sum_now
    lax.fori_loop(1, ranks, relay, 0)
    for d in range(1, cores):
        give_to(d).wait()
    lax.fori_loop(1, ranks, wait_relay, 0)


def body(ensemble, obs_cell, obs_value, obs_noise, obs_weight, tile_lists, batch_order):
    mem, levels, cells = ensemble.shape
    batches, own = obs_cell.shape
    ranks, cores = lax.axis_size("lon"), lax.axis_size("lev")
    obs = own * ranks
    own_max = 8
    slots = -(-tile_lists.shape[1] // 16) * 16
    width = -(-(-(-batches // cores) * mem) // 128) * 128
    depth = -(-own // 8) * 8
    vmem = pl.BlockSpec(memory_space=pltpu.VMEM)
    hbm = pl.BlockSpec(memory_space=pltpu.HBM)
    dma = pltpu.SemaphoreType.DMA
    landed, table = pl.pallas_call(
        functools.partial(
            gather_kernel, ranks=ranks, cores=cores, batches=batches, mem=mem, levels=levels, cells=cells,
            obs=obs, own_max=own_max,
        ),
        out_shape=[
            jax.ShapeDtypeStruct((ranks, cores, own_max, width), f32), jax.ShapeDtypeStruct((obs, 128), f32)
        ],
        in_specs=[hbm] * 5,
        out_specs=[vmem, vmem],
        scratch_shapes=[
            pltpu.VMEM((mem, levels, cells), f32),
            pltpu.VMEM((own, batches), jnp.int32),
            pltpu.VMEM((own, batches), f32),
            pltpu.VMEM((own, batches), f32),
            pltpu.VMEM((batches, levels, obs), f32),
            dma((4,)),
            pltpu.VMEM((depth, 128), f32),
            pltpu.VMEM((ranks, depth, 128), f32),
            pltpu.VMEM((cores, own_max, width), f32),
            pltpu.VMEM((cores, own_max, width), f32),
            pltpu.VMEM((own_max, width), f32),
            dma(()), dma((ranks,)), dma((ranks,)), dma((cores,)), dma((cores,)), dma((ranks,)), dma((ranks,)),
            dma((cores, ranks)), dma((cores, ranks)),
        ],
        compiler_params=pltpu.CompilerParams(
            collective_id=0, has_side_effects=True, vmem_limit_bytes=67000000
        ),
        name="gather",
    )(ensemble, obs_cell.T, obs_value.T, obs_noise.T, obs_weight)

    return pl.pallas_call(
        functools.partial(
            kernel_body, batches=batches, levels=levels, mem=mem, obs=obs, cells=cells, slots=slots,
            axis_size=ranks, own_max=own_max,
        ),
        out_shape=jax.ShapeDtypeStruct((mem, levels, cells), f32),
        in_specs=[pl.BlockSpec(memory_space=pltpu.SMEM), hbm, vmem, vmem, hbm],
        out_specs=hbm,
        scratch_shapes=[
            pltpu.VMEM((levels, mem, cells), f32),
            pltpu.VMEM((batches, mem, obs), f32),
            pltpu.VMEM((batches, mem, obs), f32),
            pltpu.VMEM((obs, obs), f32),
            pltpu.VMEM((obs, obs), f32),
            pltpu.VMEM((slots, cells), f32),
            pltpu.VMEM((slots, 3 * mem), bf16),
            pltpu.VMEM((mem, 3 * slots), bf16),
            pltpu.VMEM((128, obs), f32),
            pltpu.VMEM((batches, obs, obs), f32),
            pltpu.VMEM((batches, obs, obs), f32),
            pltpu.VMEM((batches, slots, obs), f32),
            pltpu.VMEM(tile_lists.shape, jnp.int32),
            dma(()),
            dma((levels,)),
            dma((levels,)),
        ],
        compiler_params=pltpu.CompilerParams(vmem_limit_bytes=67000000),
        name="assimilate",
    )(batch_order, ensemble, landed, table, tile_lists)


def solution(mesh):
    return jax.shard_map(
        body,
        mesh=mesh,
        in_specs=(
            P(None, "lev", "lon"),
            P(None, "lon"),
            P(None, "lon"),
            P(None, "lon"),
            P(None, "lev", None),
            P(None, "lon"),
            P(),
        ),
        out_specs=P(None, "lev", "lon"),
        check_vma=False,
    )
```

```python
import functools

import jax
import jax.numpy as jnp
from jax import lax
from jax.experimental import pallas as pl
from jax.experimental.pallas import tpu as pltpu
from jax.sharding import PartitionSpec as P

LON_DEV = 16
CELL_DEV = 1024
PANEL = 16
HALF = 8
GROUP = 2

highest = lax.Precision.HIGHEST
f32 = jnp.float32
bf16 = jnp.bfloat16


def split(x):
    high = x.astype(bf16)
    low = (x - high.astype(f32)).astype(bf16)
    return high, low


def dot(a, b):
    return jnp.dot(a, b, preferred_element_type=f32)


def tapered_weight(row_a, col_a, row_c, col_c, circle):
    e = jnp.abs(col_a - col_c)
    e = jnp.minimum(e, circle - e)
    d = row_a - row_c
    return jnp.exp((e * e + d * d) * (-2.0 / (LON_DEV * LON_DEV)))


def eliminate(a_ref, b_ref, root_ref, col_ref, two_ref, low_a, low_b, up_ref, right_ref, mem, obs, beside):
    lane = lax.broadcasted_iota(jnp.int32, (HALF, obs), 1)
    sub = lax.broadcasted_iota(jnp.int32, (HALF, obs), 0)
    sample = lane < mem

    def every(ref, row):
        return ref[pl.ds(row, HALF, stride=0), :]

    def along(rows, column):
        return jnp.broadcast_to(rows[:, column : column + 1], (HALF, obs))

    def factor_half(spot, rows, sides, first, base, end, on_pivot):
        for r in range(HALF):
            pivot = spot[r][r]
            inverse_root = lax.rsqrt(pivot)
            inverse = inverse_root * inverse_root
            root = pivot * inverse_root
            below = [spot[i][r] * inverse for i in range(r + 1, HALF)]
            for n, i in enumerate(range(r + 1, HALF)):
                for t in range(r + 1, i + 1):
                    spot[i][t] = spot[i][t] - below[n] * spot[t][r]
            added = jnp.where(sample, every(root_ref, base + r), 0.0)
            solved = sides[r] * (1.0 / (root + added))
            passing = solved * root
            for n, i in enumerate(range(r + 1, HALF)):
                rows[i] = rows[i] - below[n] * rows[r]
                sides[i] = sides[i] - below[n] * passing
            on_pivot(r, spot, inverse, rows[r], passing)
            at = first + r
            up_ref[at : at + 1, :] = rows[r][:1]
            right_ref[at : at + 1, :obs] = (rows[r] * inverse)[:1]
            right_ref[at : at + 1, obs:] = (solved * inverse_root)[:1]
            a_ref[base + r : base + r + 1, :] = jnp.where(lane < end, rows[r] * inverse_root, 0.0)[:1]
            b_ref[base + r : base + r + 1, :] = solved[:1]

    for start in range(0, obs, PANEL):
        end = start + PANEL
        middle = start + HALF
        in_panel = (lane >= start) & (lane < end)
        raw = [every(a_ref, start + i) for i in range(HALF)]
        spot = [[along(raw[i], start + t) for t in range(i + 1)] for i in range(HALF)]
        rows = [jnp.where(in_panel, jnp.where(lane == start + i, 1.0, 0.0), raw[i]) for i in range(HALF)]
        sides = [every(b_ref, start + i) for i in range(HALF)]
        rest = a_ref[middle:end, :]
        column = [along(rest, start + t) for t in range(HALF)]
        second = [along(rest, middle + t) for t in range(HALF)]
        state = [
            jnp.where(in_panel, jnp.where(lane == middle + sub, 1.0, 0.0), rest),
            b_ref[middle:end, :],
        ]

        def reach(r, spot, inverse, row, passing):
            col_ref[HALF * r : HALF * r + HALF, :] = column[r]
            scaled = column[r] * inverse
            for t in range(r + 1, HALF):
                column[t] = column[t] - scaled * spot[t][r]
            state[0] = state[0] - scaled * row
            state[1] = state[1] - scaled * passing
            for t in range(HALF):
                second[t] = second[t] - scaled * every(col_ref, HALF * r + t)

        factor_half(spot, rows, sides, 0, start, end, reach)
        for t in range(HALF):
            two_ref[HALF * t : HALF * t + HALF, :] = second[t]
        low_a[...] = state[0]
        low_b[...] = state[1]
        spot = [[every(two_ref, HALF * t + i) for t in range(i + 1)] for i in range(HALF)]
        rows = [every(low_a, i) for i in range(HALF)]
        sides = [every(low_b, i) for i in range(HALF)]
        factor_half(spot, rows, sides, HALF, middle, end, lambda *unused: None)
        beside(start // PANEL, obs // PANEL)
        if end < obs:
            u_high, u_low = split(up_ref[...])
            high, low = split(right_ref[...])
            upper = jnp.concatenate([u_high.astype(f32), u_high.astype(f32), u_low.astype(f32)], axis=0)
            left = upper.T.astype(bf16)[end:, :]
            change = dot(left, jnp.concatenate([high, low, high], axis=0))
            a_ref[end:, :] = jnp.where(
                (lane[:1] >= start) & (lane[:1] < end), 0.0, a_ref[end:, :]
            ) - change[:, :obs]
            b_ref[end:, :] = b_ref[end:, :] - change[:, obs:]


def kernel_body(
    order_ref, x_ref, landed_ref, table_ref, list_hbm, out_ref,
    state, natural, probes, a_ref, b_ref, root_ref, col_ref, two_ref, low_a, low_b, up_ref,
    right_ref, weight_ref, left_ref, gains_ref, rows_ref, noise_cols, cell_cols,
    list_cols, list_ref, sem_list, sem_in, sem_out, *, batches, levels, mem, obs, cells, slots, axis_size, own_max,
):
    def fetch(level):
        return pltpu.make_async_copy(x_ref.at[:, level, :], state.at[level], sem_in.at[level])

    def deliver(level):
        return pltpu.make_async_copy(state.at[level], out_ref.at[:, level, :], sem_out.at[level])

    list_copy = pltpu.make_async_copy(list_hbm, list_ref, sem_list)
    list_copy.start()
    for level in range(levels):
        fetch(level).start()
    tile = lax.axis_index("lon")
    circle = float(LON_DEV * axis_size)
    scale = 1.0 / (mem - 1)
    cell = lax.broadcasted_iota(jnp.int32, (1, cells), 1)
    here_row = (cell // LON_DEV).astype(f32)
    here_col = (tile * LON_DEV + cell % LON_DEV).astype(f32)
    lanes = lax.broadcasted_iota(jnp.int32, (obs, obs), 1)
    subs = lax.broadcasted_iota(jnp.int32, (obs, obs), 0)
    table = table_ref[...]
    rows = table.T
    rows_ref[...] = rows
    count = axis_size * own_max
    spot = lax.broadcasted_iota(jnp.int32, (count, obs), 0).astype(f32)
    list_copy.wait()
    listed_rows = jnp.concatenate(
        [list_ref[...].astype(f32), jnp.full((batches, obs - list_ref.shape[1]), float(obs), f32)], axis=1
    )
    listed_rows = jnp.concatenate([listed_rows, jnp.zeros((obs - batches, obs), f32)], axis=0).T
    parts = landed_ref.shape[1]
    share = -(-batches // parts)
    lane_b = lanes[:, :128]
    tile_cols = (jnp.where(lane_b < batches, table, 0.0).astype(jnp.int32) // CELL_DEV).astype(f32)
    tile_rows = tile_cols.T
    roots_all = jnp.sqrt(jnp.where((lane_b >= 2 * batches) & (lane_b < 3 * batches), table, 1.0))
    sooner = jnp.where(subs < lanes, 1.0, 0.0)
    for b in range(batches):
        tile_row = tile_rows[b : b + 1, :]
        tile_col = jnp.broadcast_to(tile_cols[:, b : b + 1], (obs, obs))
        rank = jnp.sum(jnp.where(tile_col == tile_row, sooner, 0.0), axis=0, keepdims=True)
        slot = tile_row * own_max + rank
        found = jnp.where(spot == slot, 1.0, 0.0).astype(bf16)
        first = b % share * mem
        slab = landed_ref[:, b // share, :, first : first + mem].reshape(count, mem)
        high, low = split(slab)
        left = jnp.concatenate([high.astype(f32), low.astype(f32)], axis=0).T.astype(bf16)
        natural[b] = dot(left, jnp.concatenate([found, found], axis=0))
        noise_cols[b] = jnp.broadcast_to(roots_all[:, 2 * batches + b : 2 * batches + b + 1], (obs, obs))
        cell_cols[b] = jnp.broadcast_to(table[:, b : b + 1], (obs, obs))
        list_cols[b] = jnp.broadcast_to(listed_rows[:slots, b : b + 1], (slots, obs))

    def arrange(k, carry):
        probes[k] = natural[order_ref[k]]
        return carry

    lax.fori_loop(0, batches, arrange, 0)

    def place_of(cells_now):
        cells_now = cells_now.astype(jnp.int32)
        its_tile = cells_now // CELL_DEV
        within = cells_now - its_tile * CELL_DEV
        row = within // LON_DEV
        col = its_tile * LON_DEV + within - row * LON_DEV
        return row.astype(f32), col.astype(f32), its_tile.astype(f32)

    def spread_piece(level, start, width):
        piece = pl.ds(start, width)
        block = state[level, :, piece]
        high, low = split(block)
        crossed = dot(left_ref[...], jnp.concatenate([high, low, high], axis=0))
        high, low = split(crossed * weight_ref[:, piece])
        state[level, :, piece] = block + dot(gains_ref[...], jnp.concatenate([high, low, high], axis=0))

    def beside(step, steps):
        halves = 2 * levels
        for piece in range(step * halves // steps, (step + 1) * halves // steps):
            spread_piece(piece // 2, piece % 2 * (cells // 2), cells // 2)

    def turn(k, carry):
        block = order_ref[k]
        now = probes[k]
        centre = jnp.mean(now, axis=0, keepdims=True)
        spread = now - centre
        innovation = rows_ref[pl.ds(batches + block, 1), :] - centre
        padded = jnp.concatenate(
            [spread, innovation, jnp.zeros((obs - mem - 1, obs), f32)], axis=0
        )
        sides = padded.T
        noise_row = rows_ref[pl.ds(2 * batches + block, 1), :]
        s_high, s_low = split(spread)
        stacked = jnp.concatenate([s_high.astype(f32), s_high.astype(f32), s_low.astype(f32)], axis=0)
        left = stacked.T.astype(bf16)
        covariance = dot(left, jnp.concatenate([s_high, s_low, s_high], axis=0)) * scale
        a_ref[...] = covariance + jnp.where(lanes == subs, noise_row, 0.0)
        b_ref[...] = sides
        root_ref[...] = noise_cols[block]
        eliminate(a_ref, b_ref, root_ref, col_ref, two_ref, low_a, low_b, up_ref, right_ref, mem, obs, beside)
        f_high, f_low = split(a_ref[...].T)
        b_high, b_low = split(b_ref[...])
        joined = dot(
            jnp.concatenate([f_high, f_high, f_low], axis=1), jnp.concatenate([b_high, b_low, b_high], axis=0)
        )
        gain_t = joined[:, mem : mem + 1] - joined
        gain = gain_t.T[:mem, :]

        g_high, g_low = split(gain)
        gains = jnp.concatenate([g_high, g_high, g_low], axis=1)

        from_row, from_col, from_tile = place_of(cell_cols[block])

        def renew(first):
            @pl.when(first + GROUP - 1 > k)
            def _():
                members = range(first, first + GROUP)
                upcoming = jnp.concatenate([probes[j] for j in members], axis=1)
                high, low = split(upcoming)
                crossed = dot(left, jnp.concatenate([high, low, high], axis=0))
                weights = []
                for j in members:
                    target_row, target_col, target_tile = place_of(rows_ref[pl.ds(order_ref[j], 1), :])
                    weight = tapered_weight(from_row, from_col, target_row, target_col, circle)
                    apart = jnp.abs(from_tile - target_tile)
                    near = (apart < 1.5) | (apart > axis_size - 1.5)
                    weights.append(jnp.where(near, weight * scale, 0.0))
                high, low = split(crossed * jnp.concatenate(weights, axis=1))
                upcoming = upcoming + dot(gains, jnp.concatenate([high, low, high], axis=0))
                for n, j in enumerate(members):
                    probes[j] = upcoming[:, n * obs : (n + 1) * obs]

        for first in range(0, batches, GROUP):
            renew(first)

        listed = list_cols[block]
        chosen = lanes[:slots].astype(f32) == listed
        select = chosen.astype(bf16)
        pick_row, pick_col, _ = place_of(rows_ref[pl.ds(block, 1), :])
        list_row = jnp.sum(jnp.where(chosen, pick_row, 0.0), axis=1, keepdims=True)
        list_col = jnp.sum(jnp.where(chosen, pick_col, 0.0), axis=1, keepdims=True)
        usable = jnp.where(listed[:, :1] < obs, scale, 0.0)
        weight = tapered_weight(list_row, list_col, here_row, here_col, circle) * usable
        left_listed = dot(select, left).astype(bf16)
        gt_high, gt_low = split(gain_t)
        gt_high = dot(select, gt_high)
        gt_low = dot(select, gt_low)
        gains_listed = jnp.concatenate([gt_high, gt_high, gt_low, jnp.zeros((obs - 3 * slots, obs), f32)], axis=0)
        gains_listed = gains_listed.T[:mem, : 3 * slots].astype(bf16)

        weight_ref[...] = weight
        left_ref[...] = left_listed
        gains_ref[...] = gains_listed
        return carry

    weight_ref[...] = jnp.zeros(weight_ref.shape, f32)
    left_ref[...] = jnp.zeros(left_ref.shape, bf16)
    gains_ref[...] = jnp.zeros(gains_ref.shape, bf16)
    for level in range(levels):
        fetch(level).wait()
    lax.fori_loop(0, batches, turn, 0)

    def last(level, carry):
        spread_piece(level, 0, cells)
        deliver(level).start()
        return carry

    lax.fori_loop(0, levels, last, 0)
    for level in range(levels):
        deliver(level).wait()


def gather_kernel(
    x_ref, cell_hbm, value_hbm, noise_hbm, weight_hbm, landed, table_ref,
    x_in, cell_ref, value_ref, noise_ref, weight_ref, small_sem, mine, tables, packed, partial, total, x_sem,
    table_send, table_recv, pair_send, pair_recv, send_sem, recv_sem, pass_send, pass_recv,
    *, ranks, cores, batches, mem, levels, cells, obs, own_max,
):
    lon, lev = lax.axis_index("lon"), lax.axis_index("lev")
    mesh_id = pl.DeviceIdType.MESH
    fetch = pltpu.make_async_copy(x_ref, x_in, x_sem)
    small = [
        pltpu.make_async_copy(src, dst, small_sem.at[i])
        for i, (src, dst) in enumerate(
            [(cell_hbm, cell_ref), (value_hbm, value_ref), (noise_hbm, noise_ref), (weight_hbm, weight_ref)]
        )
    ]
    for copy in small:
        copy.start()
    fetch.start()
    for copy in small[:3]:
        copy.wait()
    own = cell_ref.shape[0]
    depth = mine.shape[0]
    row = jnp.concatenate(
        [cell_ref[...].astype(f32), value_ref[...], noise_ref[...], jnp.zeros((own, 128 - 3 * batches), f32)], axis=1
    )
    if own < depth:
        row = jnp.concatenate([row, jnp.zeros((depth - own, 128), f32)], axis=0)
    mine[...] = row

    def chip(d):
        return lax.rem(lon + d, ranks), lev

    def core(d):
        return lon, lax.rem(lev + d, cores)

    barrier = pltpu.get_barrier_semaphore()

    def announce(d, carry):
        pl.semaphore_signal(barrier, inc=1, device_id=chip(d), device_id_type=mesh_id)
        return carry

    lax.fori_loop(1, ranks, announce, 0)
    for d in range(1, cores):
        pl.semaphore_signal(barrier, inc=1, device_id=core(d), device_id_type=mesh_id)
    pl.semaphore_wait(barrier, ranks + cores - 2)

    def table_to(d):
        return pltpu.make_async_remote_copy(
            src_ref=mine, dst_ref=tables.at[lon], send_sem=table_send.at[d], recv_sem=table_recv.at[d],
            device_id=chip(d), device_id_type=mesh_id,
        )

    def start_table(d, carry):
        table_to(d).start()
        return carry

    def wait_table(d, carry):
        table_to(d).wait()
        return carry

    lax.fori_loop(1, ranks, start_table, 0)
    tables[lon] = row
    lax.fori_loop(1, ranks, wait_table, 0)
    if own == depth:
        table = tables[...].reshape(obs, 128)
    else:
        table = jnp.concatenate([tables[t, :own, :] for t in range(ranks)], axis=0)
    table_ref[...] = table

    lane = lax.broadcasted_iota(jnp.int32, (obs, 128), 1)
    sub = lax.broadcasted_iota(jnp.int32, (obs, 128), 0)
    cell = jnp.where(lane < batches, table, -1.0).astype(jnp.int32)
    within = cell - lon * cells
    owned = (within >= 0) & (within < cells)
    before = jnp.where(lax.broadcasted_iota(jnp.int32, (obs, obs), 1) < lax.broadcasted_iota(jnp.int32, (obs, obs), 0), 1.0, 0.0)
    rank = dot(before.astype(bf16), jnp.where(owned, 1.0, 0.0).astype(bf16))
    code = jnp.where(owned, rank, -1.0)
    within = jnp.where(owned, within, 0)
    upper = within // LON_DEV
    lower = within - upper * LON_DEV
    deep = lax.broadcasted_iota(jnp.int32, (128, 128), 0)
    wide = lax.broadcasted_iota(jnp.int32, (128, 128), 1)
    spread_out = jnp.where((wide // own_max == deep) & (deep < batches), 1.0, 0.0).astype(bf16)
    wide_code = dot(code.astype(bf16), spread_out)
    wide_upper = dot(upper.astype(f32).astype(bf16), spread_out)
    wide_lower = dot(lower.astype(f32).astype(bf16), spread_out)
    slot = (lane - lane // own_max * own_max).astype(f32)
    taken = (wide_code == slot) & (lane < batches * own_max)
    chosen = jnp.where(taken, 1.0, 0.0)
    column = jnp.sum(jnp.where(taken, wide_upper * LON_DEV + wide_lower, 0.0), axis=0, keepdims=True)
    small[3].wait()
    weighed = jnp.dot(
        weight_ref[...].reshape(batches * levels, obs), chosen, precision=highest, preferred_element_type=f32
    )
    block_of = lax.broadcasted_iota(jnp.int32, (levels, 128), 1) // own_max
    weight = jnp.zeros((levels, 128), f32)
    for b in range(batches):
        weight = jnp.where(block_of == b, weighed[b * levels : (b + 1) * levels, :], weight)
    at = lax.broadcasted_iota(jnp.int32, (cells, 128), 0).astype(f32)
    hot = jnp.where(at == column, 1.0, 0.0).astype(bf16)
    fetch.wait()
    pieces = []
    group = 16
    for m in range(0, mem, group):
        part = x_in[m : m + group].reshape(group * levels, cells)
        high, low = split(part)
        picked = (dot(high, hot) + dot(low, hot)).reshape(group, levels, 128)
        pieces.append(jnp.sum(picked * weight[None], axis=1))
    portion = jnp.concatenate(pieces + [jnp.zeros((128 - mem, 128), f32)], axis=0).T
    share = -(-batches // cores)
    width = packed.shape[2]
    for h in range(cores):
        line = [portion[b * own_max : (b + 1) * own_max, :mem] for b in range(h * share, min((h + 1) * share, batches))]
        gap = width - len(line) * mem
        if gap:
            line.append(jnp.zeros((own_max, gap), f32))
        packed[h] = jnp.concatenate(line, axis=1)

    def pair_to(d):
        return pltpu.make_async_remote_copy(
            src_ref=packed.at[lax.rem(lev + d, cores)], dst_ref=partial.at[d], send_sem=pair_send.at[d],
            recv_sem=pair_recv.at[d], device_id=core(d), device_id_type=mesh_id,
        )

    for d in range(1, cores):
        pair_to(d).start()
    sum_now = packed[lev]
    for d in range(1, cores):
        pair_to(d).wait()
        sum_now = sum_now + partial[d]
    total[...] = sum_now

    def send_to(d):
        return pltpu.make_async_remote_copy(
            src_ref=total, dst_ref=landed.at[lon, lev], send_sem=send_sem.at[d], recv_sem=recv_sem.at[d],
            device_id=chip(d), device_id_type=mesh_id,
        )

    def give_to(d):
        return pltpu.make_async_remote_copy(
            src_ref=total, dst_ref=landed.at[lon, lev], send_sem=pass_send.at[d, 0], recv_sem=pass_recv.at[d, 0],
            device_id=core(d), device_id_type=mesh_id,
        )

    def pass_on(d, e):
        source = lax.rem(lon - d + ranks, ranks)
        return pltpu.make_async_remote_copy(
            src_ref=landed.at[source, lev], dst_ref=landed.at[source, lev], send_sem=pass_send.at[e, d],
            recv_sem=pass_recv.at[e, d], device_id=core(e), device_id_type=mesh_id,
        )

    def start_send(d, carry):
        send_to(d).start()
        return carry

    def relay(d, carry):
        send_to(d).wait()
        for e in range(1, cores):
            pass_on(d, e).start()
        return carry

    def wait_relay(d, carry):
        for e in range(1, cores):
            pass_on(d, e).wait()
        return carry

    lax.fori_loop(1, ranks, start_send, 0)
    for d in range(1, cores):
        give_to(d).start()
    landed[lon, lev] = sum_now
    lax.fori_loop(1, ranks, relay, 0)
    for d in range(1, cores):
        give_to(d).wait()
    lax.fori_loop(1, ranks, wait_relay, 0)


def body(ensemble, obs_cell, obs_value, obs_noise, obs_weight, tile_lists, batch_order):
    mem, levels, cells = ensemble.shape
    batches, own = obs_cell.shape
    ranks, cores = lax.axis_size("lon"), lax.axis_size("lev")
    obs = own * ranks
    own_max = 8
    slots = -(-tile_lists.shape[1] // 16) * 16
    width = -(-(-(-batches // cores) * mem) // 128) * 128
    depth = -(-own // 8) * 8
    vmem = pl.BlockSpec(memory_space=pltpu.VMEM)
    hbm = pl.BlockSpec(memory_space=pltpu.HBM)
    dma = pltpu.SemaphoreType.DMA
    landed, table = pl.pallas_call(
        functools.partial(
            gather_kernel, ranks=ranks, cores=cores, batches=batches, mem=mem, levels=levels, cells=cells,
            obs=obs, own_max=own_max,
        ),
        out_shape=[
            jax.ShapeDtypeStruct((ranks, cores, own_max, width), f32), jax.ShapeDtypeStruct((obs, 128), f32)
        ],
        in_specs=[hbm] * 5,
        out_specs=[vmem, vmem],
        scratch_shapes=[
            pltpu.VMEM((mem, levels, cells), f32),
            pltpu.VMEM((own, batches), jnp.int32),
            pltpu.VMEM((own, batches), f32),
            pltpu.VMEM((own, batches), f32),
            pltpu.VMEM((batches, levels, obs), f32),
            dma((4,)),
            pltpu.VMEM((depth, 128), f32),
            pltpu.VMEM((ranks, depth, 128), f32),
            pltpu.VMEM((cores, own_max, width), f32),
            pltpu.VMEM((cores, own_max, width), f32),
            pltpu.VMEM((own_max, width), f32),
            dma(()), dma((ranks,)), dma((ranks,)), dma((cores,)), dma((cores,)), dma((ranks,)), dma((ranks,)),
            dma((cores, ranks)), dma((cores, ranks)),
        ],
        compiler_params=pltpu.CompilerParams(
            collective_id=0, has_side_effects=True, vmem_limit_bytes=67000000
        ),
        name="gather",
    )(ensemble, obs_cell.T, obs_value.T, obs_noise.T, obs_weight)

    return pl.pallas_call(
        functools.partial(
            kernel_body, batches=batches, levels=levels, mem=mem, obs=obs, cells=cells, slots=slots,
            axis_size=ranks, own_max=own_max,
        ),
        out_shape=jax.ShapeDtypeStruct((mem, levels, cells), f32),
        in_specs=[pl.BlockSpec(memory_space=pltpu.SMEM), hbm, vmem, vmem, hbm],
        out_specs=hbm,
        scratch_shapes=[
            pltpu.VMEM((levels, mem, cells), f32),
            pltpu.VMEM((batches, mem, obs), f32),
            pltpu.VMEM((batches, mem, obs), f32),
            pltpu.VMEM((obs, obs), f32),
            pltpu.VMEM((obs, obs), f32),
            pltpu.VMEM((obs, obs), f32),
            pltpu.VMEM((HALF * HALF, obs), f32),
            pltpu.VMEM((HALF * HALF, obs), f32),
            pltpu.VMEM((HALF, obs), f32),
            pltpu.VMEM((HALF, obs), f32),
            pltpu.VMEM((PANEL, obs), f32),
            pltpu.VMEM((PANEL, 2 * obs), f32),
            pltpu.VMEM((slots, cells), f32),
            pltpu.VMEM((slots, 3 * mem), bf16),
            pltpu.VMEM((mem, 3 * slots), bf16),
            pltpu.VMEM((128, obs), f32),
            pltpu.VMEM((batches, obs, obs), f32),
            pltpu.VMEM((batches, obs, obs), f32),
            pltpu.VMEM((batches, slots, obs), f32),
            pltpu.VMEM(tile_lists.shape, jnp.int32),
            dma(()),
            dma((levels,)),
            dma((levels,)),
        ],
        compiler_params=pltpu.CompilerParams(vmem_limit_bytes=67000000),
        name="assimilate",
    )(batch_order, ensemble, landed, table, tile_lists)


def solution(mesh):
    return jax.shard_map(
        body,
        mesh=mesh,
        in_specs=(
            P(None, "lev", "lon"),
            P(None, "lon"),
            P(None, "lon"),
            P(None, "lon"),
            P(None, "lev", None),
            P(None, "lon"),
            P(),
        ),
        out_specs=P(None, "lev", "lon"),
        check_vma=False,
    )
```
